32 devices in a mesh: ctx: 8 (over z, y), head: 4 (over x, core).
Axes of the slice: x: 2, y: 2, z: 4, core: 2. Of those that a mesh axis runs over, the one named last changes fastest.
Arguments:
- block_order: int32 [16], replicated, may hold values from 0 to 15, as said below
- main_query: bfloat16 [1024, 36864], P('ctx', 'head'), may hold values from -256 to 256
- latent_key: bfloat16 [576, 1024], P(None, 'ctx'), may hold values from -24 to 24
- index_query: bfloat16 [1024, 32, 128], P('ctx', 'head'), may hold values from -64 to 64
- index_weight: bfloat16 [1024, 32], P('ctx', 'head'), may hold values from -0.6 to 0.6
- index_key: bfloat16 [128, 1024], P(None, 'ctx'), may hold values from -24 to 24
Outputs:
- row_loss: float32 [1024], P('ctx')
- grad_query: bfloat16 [1024, 32, 128], P('ctx', 'head')
- grad_weight: bfloat16 [1024, 32], P('ctx', 'head')
- grad_key: float32 [1024, 128], P(('ctx', 'head'))
The draws below stay inside these ranges and needn't reach their ends.
Inputs may be any that keep to these rules, and one draw needn't show every extreme that they name: `block_order`: slots 2d and 2d+1 hold blocks s * 8 + c and s * 8 + 16 // 2 - 1 - c of one sequence s, for some c below 4, and every block appears once.
All inputs are finite; a program needn't handle non-finite values.
Results may differ from the reference program's by a relative error of at most 0.01.
Values may be sent and summed in bfloat16 or wider, within the bound.
A program may use at most 128 MiB of HBM per device.

```python
import math
import jax
import jax.numpy as jnp
from jax import lax

BLOCK = 64
HM = 64
KW = 576
HEAD_QK = 192
HI = 32
DI = 128
BLOCKS = 16
LENGTH = 512
SEQ = 1024


def drawn_rows(key):
    offsets = jax.random.randint(jax.random.fold_in(key, 11), (BLOCKS,), 1, BLOCK)
    chosen_rows = jnp.arange(BLOCKS, dtype=jnp.int32) * BLOCK + offsets.astype(jnp.int32)
    level = (jnp.arange(BLOCKS, dtype=jnp.int32) % 3).astype(jnp.float32)
    target_score = 120.0 + 105.0 * level
    gap_size = 1.0 + level
    return (chosen_rows, target_score, gap_size)


def draw_block_order(key, part):
    pair_count = BLOCKS // 2
    half_pairs = pair_count // 2
    chosen = jax.random.permutation(jax.random.fold_in(key, 1), pair_count).astype(jnp.int32)
    sequence_id = chosen // half_pairs
    inner = chosen % half_pairs
    early_blocks = sequence_id * pair_count + inner
    late_blocks = sequence_id * pair_count + pair_count - 1 - inner
    return jnp.stack([early_blocks, late_blocks], axis=1).reshape(BLOCKS).astype(jnp.int32)


def draw_latent_key(key, part):
    values_drawn = jax.random.normal(jax.random.fold_in(key, 2), (KW, SEQ), jnp.float32)
    chosen_rows, target_score, gap_size = drawn_rows(key)
    anchor = 4.0 * jax.random.normal(jax.random.fold_in(key, 14), (KW, BLOCKS), jnp.float32)
    anchor = jnp.clip(anchor, -24.0, 24.0)
    spread_size = jnp.sqrt(jnp.mean(anchor * anchor, axis=0, keepdims=True))
    noise = jax.random.normal(jax.random.fold_in(key, 4), (KW, BLOCKS), jnp.float32)
    near_copy = anchor * (1.0 - gap_size / target_score)[None, :] + 0.005 * spread_size * noise
    values_drawn = values_drawn.at[:, chosen_rows].set(anchor)
    values_drawn = values_drawn.at[:, chosen_rows - 1].set(near_copy)
    return jnp.clip(values_drawn, -24.0, 24.0).astype(jnp.bfloat16)


def draw_main_query(key, part):
    values_drawn = jax.random.normal(jax.random.fold_in(key, 5), (SEQ, HM, KW), jnp.float32)
    keys_float = draw_latent_key(key, part).astype(jnp.float32)
    chosen_rows, target_score, gap_size = drawn_rows(key)
    anchor = keys_float[:, chosen_rows].T
    factor = target_score * math.sqrt(HEAD_QK)
    aligned = factor[:, None] * anchor / jnp.sum(anchor * anchor, axis=1, keepdims=True)
    values_drawn = values_drawn.at[chosen_rows].set(jnp.broadcast_to(aligned[:, None, :], (BLOCKS, HM, KW)))
    return jnp.clip(values_drawn, -256.0, 256.0).reshape(SEQ, HM * KW).astype(jnp.bfloat16)


def draw_index_key(key, part):
    values_drawn = jax.random.normal(jax.random.fold_in(key, 7), (DI, SEQ), jnp.float32)
    chosen_rows, target_score, gap_size = drawn_rows(key)
    anchor = 4.0 * jax.random.normal(jax.random.fold_in(key, 15), (DI, BLOCKS), jnp.float32)
    anchor = jnp.clip(anchor, -24.0, 24.0)
    spread_size = jnp.sqrt(jnp.mean(anchor * anchor, axis=0, keepdims=True))
    noise = jax.random.normal(jax.random.fold_in(key, 12), (DI, BLOCKS), jnp.float32)
    near_copy = anchor * (1.0 - gap_size / target_score)[None, :] + 0.005 * spread_size * noise
    values_drawn = values_drawn.at[:, chosen_rows].set(anchor)
    values_drawn = values_drawn.at[:, chosen_rows - 1].set(near_copy)
    return jnp.clip(values_drawn, -24.0, 24.0).astype(jnp.bfloat16)


def draw_index_weight(key, part):
    values_drawn = 0.1 * jax.random.normal(jax.random.fold_in(key, 9), (SEQ, HI), jnp.float32)
    return jnp.clip(values_drawn, -0.6, 0.6).astype(jnp.bfloat16)


def draw_index_query(key, part):
    values_drawn = jax.random.normal(jax.random.fold_in(key, 10), (SEQ, HI, DI), jnp.float32)
    keys_float = draw_index_key(key, part).astype(jnp.float32)
    weights = draw_index_weight(key, part).astype(jnp.float32)
    chosen_rows, target_score, gap_size = drawn_rows(key)
    anchor = keys_float[:, chosen_rows].T
    unit_part = anchor / jnp.sum(anchor * anchor, axis=1, keepdims=True)
    chosen_weights = weights[chosen_rows]
    signs = jnp.sign(chosen_weights)
    weight_total = jnp.sum(jnp.abs(chosen_weights), axis=1) + 0.001
    factor = target_score / weight_total
    aligned = factor[:, None, None] * signs[:, :, None] * unit_part[:, None, :]
    values_drawn = values_drawn.at[chosen_rows].set(aligned)
    return jnp.clip(values_drawn, -64.0, 64.0).astype(jnp.bfloat16)


def setup_inputs(seed: int = 0) -> dict:
    key_of = jax.random.split(jax.random.key(seed), 7)
    block_order = draw_block_order(jax.random.fold_in(key_of[6], 71), 0)
    main_query = draw_main_query(jax.random.fold_in(key_of[6], 71), 0)
    latent_key = draw_latent_key(jax.random.fold_in(key_of[6], 71), 0)
    index_query = draw_index_query(jax.random.fold_in(key_of[6], 71), 0)
    index_weight = draw_index_weight(jax.random.fold_in(key_of[6], 71), 0)
    index_key = draw_index_key(jax.random.fold_in(key_of[6], 71), 0)
    return dict(block_order=block_order, main_query=main_query, latent_key=latent_key, index_query=index_query, index_weight=index_weight, index_key=index_key)


masked_value = -1e+30

def reference(block_order, main_query, latent_key, index_query, index_weight, index_key):
    slot_of = jnp.argsort(block_order).astype(jnp.int32)
    offsets = jnp.arange(BLOCK, dtype=jnp.int32)
    row_sorted = (slot_of[:, None] * BLOCK + offsets[None, :]).reshape(SEQ)
    row_stored = (block_order.astype(jnp.int32)[:, None] * BLOCK + offsets[None, :]).reshape(SEQ)
    queries = main_query[row_sorted].reshape(SEQ, HM, KW)
    latent = latent_key[:, row_sorted]
    index_rows = index_query[row_sorted]
    index_weights = index_weight[row_sorted].astype(jnp.float32)
    index_keys = index_key[:, row_sorted]
    score_scale = 1.0 / math.sqrt(HEAD_QK)
    row_block = math.gcd(LENGTH, 512)
    key_grad = jnp.zeros((SEQ, DI), jnp.float32)
    loss_parts = []
    query_parts = []
    weight_parts = []
    for block_index in range(SEQ // row_block):
        first_row = block_index * row_block
        last_row = first_row + row_block
        key_first = first_row // LENGTH * LENGTH
        key_lat = latent[:, key_first:last_row]
        key_idx = index_keys[:, key_first:last_row]
        row_pos = first_row + jnp.arange(row_block, dtype=jnp.int32)
        visible = (key_first + jnp.arange(last_row - key_first, dtype=jnp.int32))[None, :] <= row_pos[:, None]

        def add_head(target_sum, query_rows):
            scores = jnp.dot(query_rows, key_lat, preferred_element_type=jnp.float32) * score_scale
            scores = jnp.where(visible, scores, masked_value)
            top_score = lax.optimization_barrier(jnp.max(scores, axis=1, keepdims=True))
            raised = jnp.exp(scores - top_score)
            return (target_sum + raised / lax.optimization_barrier(jnp.sum(raised, axis=1, keepdims=True)), None)
        target, unused = lax.scan(add_head, jnp.zeros((row_block, last_row - key_first), jnp.float32), jnp.moveaxis(queries[first_row:last_row], 1, 0))
        target = target * (1.0 / HM)
        head_rows = jnp.moveaxis(index_rows[first_row:last_row], 1, 0)
        head_weights = jnp.moveaxis(index_weights[first_row:last_row], 1, 0)

        def add_index(logit_sum, paired):
            query_rows, weight_col = paired
            activation = jnp.dot(query_rows, key_idx, preferred_element_type=jnp.float32)
            return (logit_sum + weight_col[:, None] * jnp.maximum(activation, 0.0), None)
        logits, unused = lax.scan(add_index, jnp.zeros((row_block, last_row - key_first), jnp.float32), (head_rows, head_weights))
        masked = jnp.where(visible, logits, masked_value)
        top_logit = lax.optimization_barrier(jnp.max(masked, axis=1, keepdims=True))
        log_total = top_logit + jnp.log(lax.optimization_barrier(jnp.sum(jnp.exp(masked - top_logit), axis=1, keepdims=True)))
        loss_parts.append(lax.optimization_barrier(jnp.sum(jnp.where(visible, target * (log_total - logits), 0.0), axis=1)))
        slopes = jnp.where(visible, jnp.exp(masked - log_total) - target, 0.0).astype(jnp.bfloat16)
        slope_float = lax.optimization_barrier(slopes).astype(jnp.float32)

        def back_head(key_sum, triple):
            query_rows, weight_col = triple
            activation = jnp.dot(query_rows, key_idx, preferred_element_type=jnp.float32)
            grad_weight_col = lax.optimization_barrier(jnp.sum(slope_float * jnp.maximum(activation, 0.0), axis=1))
            through = jnp.where(activation > 0.0, slope_float * weight_col[:, None], 0.0).astype(jnp.bfloat16)
            grad_rows = jnp.dot(through, key_idx.T, preferred_element_type=jnp.float32)
            key_sum = key_sum + jnp.dot(through.T, query_rows, preferred_element_type=jnp.float32)
            return (key_sum, (grad_rows, grad_weight_col))
        key_sum, outputs = lax.scan(back_head, jnp.zeros((last_row - key_first, DI), jnp.float32), (head_rows, head_weights))
        key_grad = key_grad.at[key_first:last_row].add(key_sum)
        query_parts.append(jnp.moveaxis(outputs[0], 0, 1))
        weight_parts.append(jnp.moveaxis(outputs[1], 0, 1))
    row_loss = jnp.concatenate(loss_parts)[row_stored]
    grad_query = jnp.concatenate(query_parts)[row_stored].astype(jnp.bfloat16)
    grad_weight = jnp.concatenate(weight_parts)[row_stored].astype(jnp.bfloat16)
    grad_key = key_grad[row_stored]
    return (row_loss, grad_query, grad_weight, grad_key)
```

```python
import functools
import math

import jax
import jax.numpy as jnp
from jax import lax
from jax.experimental import pallas as pl
from jax.experimental.pallas import tpu as pltpu
from jax.sharding import PartitionSpec as P

HEAD_QK = 192
LANES = 128
HALF = 64
masked_value = -1e30


def each(lower, upper, step):
    if upper - lower <= 16:
        for index in range(lower, upper):
            step(index)
    else:
        lax.fori_loop(lower, upper, lambda index, carry: (step(index), carry)[1], 0)


def total_over(upper, term):
    if upper <= 16:
        return functools.reduce(lambda a, b: a + b, [term(index) for index in range(upper)])
    return lax.fori_loop(0, upper, lambda index, carry: carry + term(index), jnp.int32(0))


def dot(a, b):
    return jnp.dot(a, b, preferred_element_type=jnp.float32)


def kernel(
    dims,
    order_ref,
    query_ref,
    latent_ref,
    rows_ref,
    weight_ref,
    index_ref,
    loss_ref,
    grad_rows_ref,
    grad_weight_ref,
    grad_key_ref,
    query_vmem,
    all_latent,
    all_index,
    window_latent,
    window_index,
    rows_turned,
    weight_col,
    act_early,
    act_late,
    part_logit,
    part_target,
    got_logit,
    got_target,
    slopes,
    losses,
    weight_grads,
    key_turned,
    key_parts,
    got_key,
    key_piece,
    key_send,
    got_piece,
    query_sem,
    index_send,
    index_recv,
    latent_send,
    latent_recv,
    logit_send,
    logit_recv,
    target_send,
    target_recv,
    slope_send,
    slope_recv,
    loss_send,
    loss_recv,
    key_send_sem,
    key_recv_sem,
    piece_send,
    piece_recv,
):
    ctx_count, head_axis, block_rows, heads, width, index_heads = dims
    pairs = ctx_count // 2
    length = ctx_count * block_rows
    early = length // 2
    quarter = block_rows // head_axis
    me = lax.axis_index("ctx")
    head = lax.axis_index("head")
    across = (head + 2) % 4
    beside = head + 1 - 2 * (head % 2)

    fetch_query = pltpu.make_async_copy(query_ref, query_vmem, query_sem)
    fetch_query.start()

    barrier = pltpu.get_barrier_semaphore()

    def greet_ctx(offset):
        pl.semaphore_signal(
            barrier, inc=1, device_id={"ctx": (me + offset) % ctx_count}, device_id_type=pl.DeviceIdType.MESH
        )

    def greet_head(offset):
        pl.semaphore_signal(
            barrier, inc=1, device_id={"head": (head + offset) % head_axis}, device_id_type=pl.DeviceIdType.MESH
        )

    each(1, ctx_count, greet_ctx)
    each(1, head_axis, greet_head)
    pl.semaphore_wait(barrier, ctx_count - 1 + head_axis - 1)

    def send(source, target, send_sem, recv_sem, where):
        return pltpu.make_async_remote_copy(
            src_ref=source,
            dst_ref=target,
            send_sem=send_sem,
            recv_sem=recv_sem,
            device_id=where,
            device_id_type=pl.DeviceIdType.MESH,
        )

    def keys_plan(own_ref, all_ref, sends, recvs):
        depth = own_ref.shape[0] // head_axis

        def piece(owner, quarter_index):
            return all_ref.at[owner, pl.ds(pl.multiple_of(quarter_index * depth, 16), depth), :]

        def first(offset):
            mine = own_ref.at[pl.ds(pl.multiple_of(head * depth, 16), depth), :]
            return send(
                mine, piece(me, head), sends.at[0, offset], recvs.at[0, offset], {"ctx": (me + offset) % ctx_count}
            )

        def onward(stage, offset):
            owner = (me + ctx_count - offset) % ctx_count
            which = across if stage == 3 else head
            where = {"head": across} if stage == 1 else {"head": beside}
            return send(
                piece(owner, which), piece(owner, which), sends.at[stage, offset], recvs.at[stage, offset], where
            )

        return first, onward

    index_first, index_onward = keys_plan(index_ref, all_index, index_send, index_recv)
    latent_first, latent_onward = keys_plan(latent_ref, all_latent, latent_send, latent_recv)
    each(1, ctx_count, lambda k: index_first(k).start())
    each(1, ctx_count, lambda k: latent_first(k).start())

    all_index[me] = index_ref[...]
    all_latent[me] = latent_ref[...]

    sequence = order_ref[2 * me] // ctx_count
    inner = order_ref[2 * me] % ctx_count

    def holder(pair):
        wanted = sequence * ctx_count + pair
        found = total_over(
            ctx_count, lambda d: jnp.where(order_ref[2 * d] == wanted, jnp.int32(1), jnp.int32(0)) * d
        )
        return jnp.minimum(found, ctx_count - 1)

    flat_rows = 2 * block_rows * index_heads
    rows_turned[...] = rows_ref[...].T
    spread = (
        lax.broadcasted_iota(jnp.int32, (flat_rows, 2 * block_rows), 0) // index_heads
        == lax.broadcasted_iota(jnp.int32, (flat_rows, 2 * block_rows), 1)
    ).astype(jnp.bfloat16)
    spread_weight = lax.dot_general(
        spread, weight_ref[...], (((1,), (1,)), ((), ())), preferred_element_type=jnp.float32
    )
    own_lane = lax.broadcasted_iota(
        jnp.int32, (flat_rows, index_heads), 0
    ) % index_heads == lax.broadcasted_iota(jnp.int32, (flat_rows, index_heads), 1)
    weight_col[...] = jnp.broadcast_to(
        jnp.sum(jnp.where(own_lane, spread_weight, 0.0), axis=1, keepdims=True), (flat_rows, LANES)
    )
    window_latent[0:HALF, :] = jnp.zeros((HALF, length), jnp.bfloat16)
    window_latent[HALF + width :, :] = jnp.zeros((HALF, length), jnp.bfloat16)

    def forward(onward):
        def one(offset):
            onward(0, offset).wait_recv()
            onward(1, offset).start()
            onward(2, offset).start()

        def two(offset):
            onward(1, offset).wait_recv()
            onward(3, offset).start()

        def three(offset):
            onward(2, offset).wait_recv()
            onward(3, offset).wait_recv()

        each(1, ctx_count, one)
        each(1, ctx_count, two)
        each(1, ctx_count, three)

    def arrange(all_ref, window_ref, top, depth):
        for pair in range(0, pairs, 2):
            a = all_ref[holder(pair)]
            b = all_ref[holder(pair + 1)]
            low = pair * block_rows
            high = length - (pair + 2) * block_rows
            window_ref[top : top + depth, low : low + LANES] = jnp.concatenate([a[:, :HALF], b[:, :HALF]], axis=1)
            window_ref[top : top + depth, high : high + LANES] = jnp.concatenate([b[:, HALF:], a[:, HALF:]], axis=1)

    chunk_rows = 16
    flat = chunk_rows * index_heads
    chunks = block_rows // chunk_rows
    sides = ((0, early, 0, act_early), (1, length, early, act_late))

    def logits_of():
        for side, columns, column_at, act_ref in sides:

            def chunk(i, carry):
                local = pl.multiple_of(i * flat, flat)
                at = pl.multiple_of(side * block_rows * index_heads + i * flat, flat)
                act = dot(rows_ref[pl.ds(at, flat), :], window_index[:, 0:columns])
                act_ref[pl.ds(local, flat), :] = act
                scaled = jnp.maximum(act, 0.0) * weight_col[pl.ds(at, flat), 0:1]
                part_logit[pl.ds(pl.multiple_of(i * chunk_rows, chunk_rows), chunk_rows), column_at : column_at + columns] = (
                    jnp.sum(scaled.reshape(chunk_rows, index_heads, columns), axis=1)
                )
                return carry

            lax.fori_loop(0, chunks, chunk, 0)

    def visible_of(side, rows, row_at, columns):
        block = jnp.where(side == 0, inner, ctx_count - 1 - inner)
        row_pos = block * block_rows + row_at + lax.broadcasted_iota(jnp.int32, (rows, columns), 0)
        return lax.broadcasted_iota(jnp.int32, (rows, columns), 1) <= row_pos

    def share(part_ref, got_ref, sends, recvs, offset):
        peer = (head + offset) % head_axis
        return send(
            part_ref.at[pl.ds(pl.multiple_of(peer * quarter, quarter), quarter), :],
            got_ref.at[offset],
            sends.at[offset],
            recvs.at[offset],
            {"head": peer},
        )

    score_scale = 1.0 / math.sqrt(HEAD_QK)
    group = max(1, min(heads // 2, 2048 // length))
    groups = heads // 2 // group
    padded = width + HALF

    def attention():
        part_target[...] = jnp.zeros(part_target.shape, jnp.float32)
        for parity in range(2):
            top = HALF if parity == 0 else 0
            lane_at = 0 if parity == 0 else width - HALF
            for side, columns, column_at, unused in sides:
                visible = visible_of(side, block_rows, 0, columns)

                def run(i, carry):
                    stacked = jnp.concatenate(
                        [
                            query_vmem[
                                side * block_rows : (side + 1) * block_rows,
                                pl.ds(pl.multiple_of((i * group + g) * 2 * width + lane_at, LANES), padded),
                            ]
                            for g in range(group)
                        ],
                        axis=0,
                    )
                    scores = dot(stacked, window_latent[top : top + padded, 0:columns]) * score_scale
                    total = part_target[:, column_at : column_at + columns]
                    for g in range(group):
                        one = jnp.where(visible, scores[g * block_rows : (g + 1) * block_rows], masked_value)
                        raised = jnp.exp(one - jnp.max(one, axis=1, keepdims=True))
                        total = total + raised * (1.0 / jnp.sum(raised, axis=1, keepdims=True))
                    part_target[:, column_at : column_at + columns] = total
                    return carry

                lax.fori_loop(0, groups, run, 0)

    forward(index_onward)
    arrange(all_index, window_index, 0, index_ref.shape[0])
    logits_of()
    each(1, head_axis, lambda k: share(part_logit, got_logit, logit_send, logit_recv, k).start())
    forward(latent_onward)
    arrange(all_latent, window_latent, HALF, width)
    fetch_query.wait()
    attention()
    each(1, head_axis, lambda k: share(part_target, got_target, target_send, target_recv, k).start())
    each(1, head_axis, lambda k: share(part_logit, got_logit, logit_send, logit_recv, k).wait_recv())
    each(1, head_axis, lambda k: share(part_target, got_target, target_send, target_recv, k).wait_recv())

    my_rows = pl.ds(pl.multiple_of(head * quarter, quarter), quarter)
    for side, columns, column_at, unused in sides:
        at = slice(column_at, column_at + columns)
        visible = visible_of(side, quarter, head * quarter, columns)
        logit = part_logit[my_rows, at]
        target = part_target[my_rows, at]
        for k in range(1, head_axis):
            logit = logit + got_logit[k, :, at]
            target = target + got_target[k, :, at]
        target = target * (1.0 / (heads * head_axis))
        masked = jnp.where(visible, logit, masked_value)
        top = jnp.max(masked, axis=1, keepdims=True)
        lse = top + jnp.log(jnp.sum(jnp.exp(masked - top), axis=1, keepdims=True))
        loss = jnp.sum(jnp.where(visible, target * (lse - logit), 0.0), axis=1, keepdims=True)
        slopes[my_rows, at] = jnp.where(visible, jnp.exp(masked - lse) - target, 0.0).astype(jnp.bfloat16)
        losses[head, side] = jnp.broadcast_to(loss, (quarter, LANES))

    def spread_slopes(offset):
        return send(
            slopes.at[my_rows, :],
            slopes.at[my_rows, :],
            slope_send.at[offset],
            slope_recv.at[offset],
            {"head": (head + offset) % head_axis},
        )

    def spread_losses(offset):
        return send(
            losses.at[head],
            losses.at[head],
            loss_send.at[offset],
            loss_recv.at[offset],
            {"head": (head + offset) % head_axis},
        )

    each(1, head_axis, lambda k: spread_slopes(k).start())
    each(1, head_axis, lambda k: spread_losses(k).start())
    each(1, head_axis, lambda k: spread_slopes(k).wait_recv())

    key_turned[...] = jnp.zeros(key_turned.shape, jnp.float32)
    lane_of = lax.broadcasted_iota(jnp.int32, (flat, LANES), 1)
    lane_own = lane_of == lax.broadcasted_iota(jnp.int32, (flat, LANES), 0) % index_heads
    for side, columns, column_at, act_ref in sides:

        def chunk(i, carry):
            local = pl.multiple_of(i * flat, flat)
            at = pl.multiple_of(side * block_rows * index_heads + i * flat, flat)
            rows_at = pl.multiple_of(i * chunk_rows, chunk_rows)
            act = act_ref[pl.ds(local, flat), :]
            slope = slopes[pl.ds(rows_at, chunk_rows), column_at : column_at + columns].astype(jnp.float32)
            slope = jnp.broadcast_to(slope[:, None, :], (chunk_rows, index_heads, columns)).reshape(flat, columns)
            col = jnp.sum(slope * jnp.maximum(act, 0.0), axis=1, keepdims=True)
            placed = jnp.where(lane_own, col, 0.0).reshape(chunk_rows, index_heads, LANES)
            weight_at = pl.multiple_of(side * block_rows + i * chunk_rows, chunk_rows)
            weight_grads[pl.ds(weight_at, chunk_rows), :] = jnp.sum(placed, axis=1)
            through = jnp.where(act > 0.0, slope * weight_col[pl.ds(at, flat), 0:1], 0.0).astype(jnp.bfloat16)
            grad_rows_ref[pl.ds(at, flat), :] = lax.dot_general(
                through,
                window_index[:, 0:columns],
                (((1,), (1,)), ((), ())),
                preferred_element_type=jnp.float32,
            ).astype(jnp.bfloat16)
            key_turned[:, 0:columns] += dot(rows_turned[:, pl.ds(at, flat)], through)
            return carry

        lax.fori_loop(0, chunks, chunk, 0)

    slot_rows = 2 * block_rows // head_axis
    grad_weight_ref[...] = weight_grads[...].T[0:index_heads].astype(jnp.bfloat16)
    for pair in range(pairs):
        low = pair * block_rows
        high = length - (pair + 1) * block_rows
        for part, start in ((0, low), (2, high)):
            lanes_at = start // LANES * LANES
            turned = key_turned[:, lanes_at : lanes_at + LANES].T
            for k in range(2):
                begin = start - lanes_at + k * slot_rows
                key_parts[part + k, pair] = turned[begin : begin + slot_rows]

    def share_key(offset):
        peer = (head + offset) % head_axis
        return send(
            key_parts.at[peer], got_key.at[offset], key_send_sem.at[offset], key_recv_sem.at[offset], {"head": peer}
        )

    each(1, head_axis, lambda k: share_key(k).start())
    each(1, head_axis, lambda k: spread_losses(k).wait_recv())
    loss_block = jnp.concatenate(
        [losses[q, side] for side in range(2) for q in range(head_axis)], axis=0
    )
    diagonal = lax.broadcasted_iota(jnp.int32, loss_block.shape, 0) == lax.broadcasted_iota(
        jnp.int32, loss_block.shape, 1
    )
    loss_ref[...] = jnp.sum(jnp.where(diagonal, loss_block, 0.0), axis=0, keepdims=True)
    each(1, head_axis, lambda k: share_key(k).wait_recv())
    for pair in range(pairs):
        piece = key_parts[head, pair]
        for k in range(1, head_axis):
            piece = piece + got_key[k, pair]
        key_piece[pair] = piece

    def fill(d):
        block = order_ref[2 * d]
        same = block // ctx_count == sequence
        key_send[d] = jnp.where(same, key_piece[block % ctx_count], 0.0)

    each(0, ctx_count, fill)

    def share_piece(offset):
        peer = (me + offset) % ctx_count
        return send(
            key_send.at[peer], got_piece.at[offset], piece_send.at[offset], piece_recv.at[offset], {"ctx": peer}
        )

    each(1, ctx_count, lambda k: share_piece(k).start())
    grad_key_ref[...] = key_send[me]

    def add(offset):
        share_piece(offset).wait_recv()
        grad_key_ref[...] += got_piece[offset]

    each(1, ctx_count, add)

    def finish_ctx(offset):
        index_first(offset).wait_send()
        latent_first(offset).wait_send()
        for stage in range(1, 4):
            index_onward(stage, offset).wait_send()
            latent_onward(stage, offset).wait_send()
        share_piece(offset).wait_send()

    def finish_head(offset):
        share(part_logit, got_logit, logit_send, logit_recv, offset).wait_send()
        share(part_target, got_target, target_send, target_recv, offset).wait_send()
        spread_slopes(offset).wait_send()
        spread_losses(offset).wait_send()
        share_key(offset).wait_send()

    each(1, ctx_count, finish_ctx)
    each(1, head_axis, finish_head)


def body(block_order, main_query, latent_key, index_query, index_weight, index_key):
    ctx_count = lax.axis_size("ctx")
    head_axis = lax.axis_size("head")
    local_rows = main_query.shape[0]
    block_rows = local_rows // 2
    width = latent_key.shape[0]
    heads = main_query.shape[1] // width
    index_heads, index_width = index_query.shape[1:]
    length = ctx_count * block_rows
    early = length // 2
    packed = early + length
    pairs = ctx_count // 2
    quarter = block_rows // head_axis
    slot_rows = local_rows // head_axis
    flat_rows = local_rows * index_heads
    f32, bf16 = jnp.float32, jnp.bfloat16
    vmem = pl.BlockSpec(memory_space=pltpu.VMEM)
    dma = pltpu.SemaphoreType.DMA
    loss, grad_rows, grad_weight, grad_key = pl.pallas_call(
        functools.partial(kernel, (ctx_count, head_axis, block_rows, heads, width, index_heads)),
        out_shape=(
            jax.ShapeDtypeStruct((1, local_rows), f32),
            jax.ShapeDtypeStruct((flat_rows, index_width), bf16),
            jax.ShapeDtypeStruct((index_heads, local_rows), bf16),
            jax.ShapeDtypeStruct((slot_rows, index_width), f32),
        ),
        in_specs=[
            pl.BlockSpec(memory_space=pltpu.SMEM),
            pl.BlockSpec(memory_space=pl.ANY),
            vmem,
            vmem,
            vmem,
            vmem,
        ],
        out_specs=(vmem, vmem, vmem, vmem),
        scratch_shapes=[
            pltpu.VMEM(main_query.shape, bf16),
            pltpu.VMEM((ctx_count,) + latent_key.shape, bf16),
            pltpu.VMEM((ctx_count,) + index_key.shape, bf16),
            pltpu.VMEM((width + 2 * HALF, length), bf16),
            pltpu.VMEM((index_width, length), bf16),
            pltpu.VMEM((index_width, flat_rows), bf16),
            pltpu.VMEM((flat_rows, LANES), f32),
            pltpu.VMEM((flat_rows // 2, early), f32),
            pltpu.VMEM((flat_rows // 2, length), f32),
            pltpu.VMEM((block_rows, packed), f32),
            pltpu.VMEM((block_rows, packed), f32),
            pltpu.VMEM((head_axis, quarter, packed), f32),
            pltpu.VMEM((head_axis, quarter, packed), f32),
            pltpu.VMEM((block_rows, packed), bf16),
            pltpu.VMEM((head_axis, 2, quarter, LANES), f32),
            pltpu.VMEM((local_rows, LANES), f32),
            pltpu.VMEM((index_width, length), f32),
            pltpu.VMEM((head_axis, pairs, slot_rows, index_width), f32),
            pltpu.VMEM((head_axis, pairs, slot_rows, index_width), f32),
            pltpu.VMEM((pairs, slot_rows, index_width), f32),
            pltpu.VMEM((ctx_count, slot_rows, index_width), f32),
            pltpu.VMEM((ctx_count, slot_rows, index_width), f32),
            dma,
            dma((4, ctx_count)),
            dma((4, ctx_count)),
            dma((4, ctx_count)),
            dma((4, ctx_count)),
        ]
        + [dma((head_axis,))] * 10
        + [dma((ctx_count,))] * 2,
        compiler_params=pltpu.CompilerParams(
            collective_id=0, has_side_effects=True, vmem_limit_bytes=60 * 1024 * 1024
        ),
    )(
        block_order,
        main_query,
        latent_key,
        index_query.reshape(flat_rows, index_width),
        index_weight.T,
        index_key,
    )
    return (
        loss.reshape(local_rows),
        grad_rows.reshape(local_rows, index_heads, index_width),
        grad_weight.T,
        grad_key,
    )


def solution(mesh):
    in_specs = (
        P(),
        P("ctx", "head"),
        P(None, "ctx"),
        P("ctx", "head", None),
        P("ctx", "head"),
        P(None, "ctx"),
    )
    out_specs = (P("ctx"), P("ctx", "head", None), P("ctx", "head"), P(("ctx", "head"), None))
    return jax.shard_map(body, mesh=mesh, in_specs=in_specs, out_specs=out_specs, check_vma=False)
```

```python
import functools
import math

import jax
import jax.numpy as jnp
from jax import lax
from jax.experimental import pallas as pl
from jax.experimental.pallas import tpu as pltpu
from jax.sharding import PartitionSpec as P

HEAD_QK = 192
LANES = 128
HALF = 64
masked_value = -1e30


def each(lower, upper, step):
    if upper - lower <= 16:
        for index in range(lower, upper):
            step(index)
    else:
        lax.fori_loop(lower, upper, lambda index, carry: (step(index), carry)[1], 0)


def total_over(upper, term):
    if upper <= 16:
        return functools.reduce(lambda a, b: a + b, [term(index) for index in range(upper)])
    return lax.fori_loop(0, upper, lambda index, carry: carry + term(index), jnp.int32(0))


def dot(a, b):
    return jnp.dot(a, b, preferred_element_type=jnp.float32)


def kernel(
    dims,
    order_ref,
    query_ref,
    latent_in,
    rows_in,
    weight_ref,
    index_in,
    loss_ref,
    grad_rows_ref,
    grad_weight_ref,
    grad_key_ref,
    query_vmem,
    rows_ref,
    through_early,
    through_late,
    all_latent,
    all_index,
    window_latent,
    window_index,
    rows_turned,
    weight_col,
    act_early,
    act_late,
    part_logit,
    part_target,
    got_logit,
    got_target,
    slopes,
    losses,
    weight_grads,
    key_turned,
    key_parts,
    got_key,
    key_piece,
    key_send,
    got_piece,
    query_sem,
    input_sem,
    index_send,
    index_recv,
    latent_send,
    latent_recv,
    logit_send,
    logit_recv,
    target_send,
    target_recv,
    slope_send,
    slope_recv,
    loss_send,
    loss_recv,
    key_send_sem,
    key_recv_sem,
    piece_send,
    piece_recv,
):
    ctx_count, head_axis, block_rows, heads, width, index_heads = dims
    pairs = ctx_count // 2
    length = ctx_count * block_rows
    early = length // 2
    quarter = block_rows // head_axis
    me = lax.axis_index("ctx")
    head = lax.axis_index("head")
    across = (head + 2) % 4
    beside = head + 1 - 2 * (head % 2)

    fetch_query = pltpu.make_async_copy(query_ref, query_vmem, query_sem)
    fetch_inputs = [
        pltpu.make_async_copy(index_in, all_index.at[me], input_sem.at[0]),
        pltpu.make_async_copy(latent_in, all_latent.at[me], input_sem.at[1]),
        pltpu.make_async_copy(rows_in, rows_ref, input_sem.at[2]),
    ]
    for fetch in fetch_inputs:
        fetch.start()
    fetch_query.start()

    barrier = pltpu.get_barrier_semaphore()

    def greet_ctx(offset):
        pl.semaphore_signal(
            barrier, inc=1, device_id={"ctx": (me + offset) % ctx_count}, device_id_type=pl.DeviceIdType.MESH
        )

    def greet_head(offset):
        pl.semaphore_signal(
            barrier, inc=1, device_id={"head": (head + offset) % head_axis}, device_id_type=pl.DeviceIdType.MESH
        )

    each(1, ctx_count, greet_ctx)
    each(1, head_axis, greet_head)
    pl.semaphore_wait(barrier, ctx_count - 1 + head_axis - 1)

    def send(source, target, send_sem, recv_sem, where):
        return pltpu.make_async_remote_copy(
            src_ref=source,
            dst_ref=target,
            send_sem=send_sem,
            recv_sem=recv_sem,
            device_id=where,
            device_id_type=pl.DeviceIdType.MESH,
        )

    def keys_plan(all_ref, sends, recvs):
        depth = all_ref.shape[1] // head_axis

        def piece(owner, quarter_index):
            return all_ref.at[owner, pl.ds(pl.multiple_of(quarter_index * depth, 16), depth), :]

        def first(offset):
            where = {"ctx": (me + offset) % ctx_count}
            return send(piece(me, head), piece(me, head), sends.at[0, offset], recvs.at[0, offset], where)

        def onward(stage, offset):
            owner = (me + ctx_count - offset) % ctx_count
            which = across if stage == 3 else head
            where = {"head": across} if stage == 1 else {"head": beside}
            return send(
                piece(owner, which), piece(owner, which), sends.at[stage, offset], recvs.at[stage, offset], where
            )

        return first, onward

    index_first, index_onward = keys_plan(all_index, index_send, index_recv)
    latent_first, latent_onward = keys_plan(all_latent, latent_send, latent_recv)
    fetch_inputs[0].wait()
    each(1, ctx_count, lambda k: index_first(k).start())
    fetch_inputs[1].wait()
    each(1, ctx_count, lambda k: latent_first(k).start())
    fetch_inputs[2].wait()

    sequence = order_ref[2 * me] // ctx_count
    inner = order_ref[2 * me] % ctx_count

    def holder(pair):
        wanted = sequence * ctx_count + pair
        found = total_over(
            ctx_count, lambda d: jnp.where(order_ref[2 * d] == wanted, jnp.int32(1), jnp.int32(0)) * d
        )
        return jnp.minimum(found, ctx_count - 1)

    flat_rows = 2 * block_rows * index_heads
    rows_turned[...] = rows_ref[...].T
    spread = (
        lax.broadcasted_iota(jnp.int32, (flat_rows, 2 * block_rows), 0) // index_heads
        == lax.broadcasted_iota(jnp.int32, (flat_rows, 2 * block_rows), 1)
    ).astype(jnp.bfloat16)
    spread_weight = lax.dot_general(
        spread, weight_ref[...], (((1,), (1,)), ((), ())), preferred_element_type=jnp.float32
    )
    own_lane = lax.broadcasted_iota(
        jnp.int32, (flat_rows, index_heads), 0
    ) % index_heads == lax.broadcasted_iota(jnp.int32, (flat_rows, index_heads), 1)
    weight_col[...] = jnp.broadcast_to(
        jnp.sum(jnp.where(own_lane, spread_weight, 0.0), axis=1, keepdims=True), (flat_rows, LANES)
    )
    window_latent[0:HALF, :] = jnp.zeros((HALF, length), jnp.bfloat16)
    window_latent[HALF + width :, :] = jnp.zeros((HALF, length), jnp.bfloat16)

    def pass_first(onward, offset):
        onward(0, offset).wait_recv()
        onward(1, offset).start()
        onward(2, offset).start()

    def pass_second(onward, offset):
        onward(1, offset).wait_recv()
        onward(3, offset).start()

    def take_last(onward, offset):
        onward(2, offset).wait_recv()
        onward(3, offset).wait_recv()

    def arrange(all_ref, window_ref, top, depth):
        for pair in range(0, pairs, 2):
            a = all_ref[holder(pair)]
            b = all_ref[holder(pair + 1)]
            low = pair * block_rows
            high = length - (pair + 2) * block_rows
            window_ref[top : top + depth, low : low + LANES] = jnp.concatenate([a[:, :HALF], b[:, :HALF]], axis=1)
            window_ref[top : top + depth, high : high + LANES] = jnp.concatenate([b[:, HALF:], a[:, HALF:]], axis=1)

    chunk_rows = 16
    flat = chunk_rows * index_heads
    chunks = block_rows // chunk_rows
    sides = ((0, early, 0, act_early, through_early), (1, length, early, act_late, through_late))

    def logits_of():
        for side, columns, column_at, act_ref, unused in sides:

            def chunk(i, carry):
                local = pl.multiple_of(i * flat, flat)
                at = pl.multiple_of(side * block_rows * index_heads + i * flat, flat)
                act = dot(rows_ref[pl.ds(at, flat), :], window_index[:, 0:columns])
                act_ref[pl.ds(local, flat), :] = act
                scaled = jnp.maximum(act, 0.0) * weight_col[pl.ds(at, flat), 0:1]
                part_logit[pl.ds(pl.multiple_of(i * chunk_rows, chunk_rows), chunk_rows), column_at : column_at + columns] = (
                    jnp.sum(scaled.reshape(chunk_rows, index_heads, columns), axis=1)
                )
                return carry

            lax.fori_loop(0, chunks, chunk, 0)

    def visible_of(side, rows, row_at, columns):
        block = jnp.where(side == 0, inner, ctx_count - 1 - inner)
        row_pos = block * block_rows + row_at + lax.broadcasted_iota(jnp.int32, (rows, columns), 0)
        return lax.broadcasted_iota(jnp.int32, (rows, columns), 1) <= row_pos

    def share(part_ref, got_ref, sends, recvs, offset):
        peer = (head + offset) % head_axis
        return send(
            part_ref.at[pl.ds(pl.multiple_of(peer * quarter, quarter), quarter), :],
            got_ref.at[offset],
            sends.at[offset],
            recvs.at[offset],
            {"head": peer},
        )

    score_scale = 1.0 / math.sqrt(HEAD_QK)
    group = max(1, min(heads // 2, 2048 // length))
    groups = heads // 2 // group
    padded = width + HALF

    def attention():
        part_target[...] = jnp.zeros(part_target.shape, jnp.float32)
        for parity in range(2):
            top = HALF if parity == 0 else 0
            lane_at = 0 if parity == 0 else width - HALF
            for side, columns, column_at, unused, unused in sides:
                visible = visible_of(side, block_rows, 0, columns)

                def run(i, carry):
                    stacked = jnp.concatenate(
                        [
                            query_vmem[
                                side * block_rows : (side + 1) * block_rows,
                                pl.ds(pl.multiple_of((i * group + g) * 2 * width + lane_at, LANES), padded),
                            ]
                            for g in range(group)
                        ],
                        axis=0,
                    )
                    scores = dot(stacked, window_latent[top : top + padded, 0:columns]) * score_scale
                    total = part_target[:, column_at : column_at + columns]
                    for g in range(group):
                        one = jnp.where(visible, scores[g * block_rows : (g + 1) * block_rows], masked_value)
                        raised = jnp.exp(one - jnp.max(one, axis=1, keepdims=True))
                        total = total + raised * (1.0 / jnp.sum(raised, axis=1, keepdims=True))
                    part_target[:, column_at : column_at + columns] = total
                    return carry

                lax.fori_loop(0, groups, run, 0)

    each(1, ctx_count, lambda k: pass_first(index_onward, k))
    each(1, ctx_count, lambda k: pass_first(latent_onward, k))
    each(1, ctx_count, lambda k: pass_second(index_onward, k))
    each(1, ctx_count, lambda k: take_last(index_onward, k))
    arrange(all_index, window_index, 0, window_index.shape[0])
    logits_of()
    each(1, head_axis, lambda k: share(part_logit, got_logit, logit_send, logit_recv, k).start())
    each(1, ctx_count, lambda k: pass_second(latent_onward, k))
    each(1, ctx_count, lambda k: take_last(latent_onward, k))
    arrange(all_latent, window_latent, HALF, width)
    fetch_query.wait()
    attention()
    each(1, head_axis, lambda k: share(part_target, got_target, target_send, target_recv, k).start())
    each(1, head_axis, lambda k: share(part_logit, got_logit, logit_send, logit_recv, k).wait_recv())
    each(1, head_axis, lambda k: share(part_target, got_target, target_send, target_recv, k).wait_recv())

    my_rows = pl.ds(pl.multiple_of(head * quarter, quarter), quarter)
    for side, columns, column_at, unused, unused in sides:
        at = slice(column_at, column_at + columns)
        visible = visible_of(side, quarter, head * quarter, columns)
        logit = part_logit[my_rows, at]
        target = part_target[my_rows, at]
        for k in range(1, head_axis):
            logit = logit + got_logit[k, :, at]
            target = target + got_target[k, :, at]
        target = target * (1.0 / (heads * head_axis))
        masked = jnp.where(visible, logit, masked_value)
        top = jnp.max(masked, axis=1, keepdims=True)
        lse = top + jnp.log(jnp.sum(jnp.exp(masked - top), axis=1, keepdims=True))
        loss = jnp.sum(jnp.where(visible, target * (lse - logit), 0.0), axis=1, keepdims=True)
        slopes[my_rows, at] = jnp.where(visible, jnp.exp(masked - lse) - target, 0.0).astype(jnp.bfloat16)
        losses[head, side] = jnp.broadcast_to(loss, (quarter, LANES))

    def spread_slopes(offset):
        return send(
            slopes.at[my_rows, :],
            slopes.at[my_rows, :],
            slope_send.at[offset],
            slope_recv.at[offset],
            {"head": (head + offset) % head_axis},
        )

    def spread_losses(offset):
        return send(
            losses.at[head],
            losses.at[head],
            loss_send.at[offset],
            loss_recv.at[offset],
            {"head": (head + offset) % head_axis},
        )

    each(1, head_axis, lambda k: spread_slopes(k).start())
    each(1, head_axis, lambda k: spread_losses(k).start())
    each(1, head_axis, lambda k: spread_slopes(k).wait_recv())

    key_turned[...] = jnp.zeros(key_turned.shape, jnp.float32)
    lane_of = lax.broadcasted_iota(jnp.int32, (flat, LANES), 1)
    lane_own = lane_of == lax.broadcasted_iota(jnp.int32, (flat, LANES), 0) % index_heads
    def slope_of(rows_at, column_at, columns):
        slope = slopes[pl.ds(rows_at, chunk_rows), column_at : column_at + columns].astype(jnp.float32)
        return jnp.broadcast_to(slope[:, None, :], (chunk_rows, index_heads, columns)).reshape(flat, columns)

    for side, columns, column_at, act_ref, through_ref in sides:

        def chunk(i, carry):
            local = pl.multiple_of(i * flat, flat)
            at = pl.multiple_of(side * block_rows * index_heads + i * flat, flat)
            rows_at = pl.multiple_of(i * chunk_rows, chunk_rows)
            act = act_ref[pl.ds(local, flat), :]
            slope = slope_of(rows_at, column_at, columns)
            through = jnp.where(act > 0.0, slope * weight_col[pl.ds(at, flat), 0:1], 0.0).astype(jnp.bfloat16)
            through_ref[pl.ds(local, flat), :] = through
            key_turned[:, 0:columns] += dot(rows_turned[:, pl.ds(at, flat)], through)
            return carry

        lax.fori_loop(0, chunks, chunk, 0)

    def row_grads():
        for side, columns, column_at, act_ref, through_ref in sides:

            def chunk(i, carry):
                local = pl.multiple_of(i * flat, flat)
                at = pl.multiple_of(side * block_rows * index_heads + i * flat, flat)
                rows_at = pl.multiple_of(i * chunk_rows, chunk_rows)
                slope = slope_of(rows_at, column_at, columns)
                col = jnp.sum(slope * jnp.maximum(act_ref[pl.ds(local, flat), :], 0.0), axis=1, keepdims=True)
                placed = jnp.where(lane_own, col, 0.0).reshape(chunk_rows, index_heads, LANES)
                weight_at = pl.multiple_of(side * block_rows + i * chunk_rows, chunk_rows)
                weight_grads[pl.ds(weight_at, chunk_rows), :] = jnp.sum(placed, axis=1)
                grad_rows_ref[pl.ds(at, flat), :] = lax.dot_general(
                    through_ref[pl.ds(local, flat), :],
                    window_index[:, 0:columns],
                    (((1,), (1,)), ((), ())),
                    preferred_element_type=jnp.float32,
                ).astype(jnp.bfloat16)
                return carry

            lax.fori_loop(0, chunks, chunk, 0)
        grad_weight_ref[...] = weight_grads[...].T[0:index_heads].astype(jnp.bfloat16)

    slot_rows = 2 * block_rows // head_axis
    for pair in range(pairs):
        low = pair * block_rows
        high = length - (pair + 1) * block_rows
        for part, start in ((0, low), (2, high)):
            lanes_at = start // LANES * LANES
            turned = key_turned[:, lanes_at : lanes_at + LANES].T
            for k in range(2):
                begin = start - lanes_at + k * slot_rows
                key_parts[part + k, pair] = turned[begin : begin + slot_rows]

    def share_key(offset):
        peer = (head + offset) % head_axis
        return send(
            key_parts.at[peer], got_key.at[offset], key_send_sem.at[offset], key_recv_sem.at[offset], {"head": peer}
        )

    each(1, head_axis, lambda k: share_key(k).start())
    row_grads()
    each(1, head_axis, lambda k: spread_losses(k).wait_recv())
    loss_block = jnp.concatenate(
        [losses[q, side] for side in range(2) for q in range(head_axis)], axis=0
    )
    diagonal = lax.broadcasted_iota(jnp.int32, loss_block.shape, 0) == lax.broadcasted_iota(
        jnp.int32, loss_block.shape, 1
    )
    loss_ref[...] = jnp.sum(jnp.where(diagonal, loss_block, 0.0), axis=0, keepdims=True)
    each(1, head_axis, lambda k: share_key(k).wait_recv())
    for pair in range(pairs):
        piece = key_parts[head, pair]
        for k in range(1, head_axis):
            piece = piece + got_key[k, pair]
        key_piece[pair] = piece

    def fill(d):
        block = order_ref[2 * d]
        same = block // ctx_count == sequence
        key_send[d] = jnp.where(same, key_piece[block % ctx_count], 0.0)

    each(0, ctx_count, fill)

    def share_piece(offset):
        peer = (me + offset) % ctx_count
        return send(
            key_send.at[peer], got_piece.at[offset], piece_send.at[offset], piece_recv.at[offset], {"ctx": peer}
        )

    each(1, ctx_count, lambda k: share_piece(k).start())
    grad_key_ref[...] = key_send[me]

    def add(offset):
        share_piece(offset).wait_recv()
        grad_key_ref[...] += got_piece[offset]

    each(1, ctx_count, add)

    def finish_ctx(offset):
        index_first(offset).wait_send()
        latent_first(offset).wait_send()
        for stage in range(1, 4):
            index_onward(stage, offset).wait_send()
            latent_onward(stage, offset).wait_send()
        share_piece(offset).wait_send()

    def finish_head(offset):
        share(part_logit, got_logit, logit_send, logit_recv, offset).wait_send()
        share(part_target, got_target, target_send, target_recv, offset).wait_send()
        spread_slopes(offset).wait_send()
        spread_losses(offset).wait_send()
        share_key(offset).wait_send()

    each(1, ctx_count, finish_ctx)
    each(1, head_axis, finish_head)


def hand_over(*refs):
    count = len(refs) // 2
    for source, target in zip(refs[:count], refs[count:]):
        target[...] = source[...]


def body(block_order, main_query, latent_key, index_query, index_weight, index_key):
    ctx_count = lax.axis_size("ctx")
    head_axis = lax.axis_size("head")
    local_rows = main_query.shape[0]
    block_rows = local_rows // 2
    width = latent_key.shape[0]
    heads = main_query.shape[1] // width
    index_heads, index_width = index_query.shape[1:]
    length = ctx_count * block_rows
    early = length // 2
    packed = early + length
    pairs = ctx_count // 2
    quarter = block_rows // head_axis
    slot_rows = local_rows // head_axis
    flat_rows = local_rows * index_heads
    f32, bf16 = jnp.float32, jnp.bfloat16
    vmem = pl.BlockSpec(memory_space=pltpu.VMEM)
    hbm = pl.BlockSpec(memory_space=pl.ANY)
    dma = pltpu.SemaphoreType.DMA
    results = pl.pallas_call(
        functools.partial(kernel, (ctx_count, head_axis, block_rows, heads, width, index_heads)),
        out_shape=(
            jax.ShapeDtypeStruct((1, local_rows), f32),
            jax.ShapeDtypeStruct((flat_rows, index_width), bf16),
            jax.ShapeDtypeStruct((index_heads, local_rows), bf16),
            jax.ShapeDtypeStruct((slot_rows, index_width), f32),
        ),
        in_specs=[
            pl.BlockSpec(memory_space=pltpu.SMEM),
            hbm,
            hbm,
            hbm,
            vmem,
            hbm,
        ],
        out_specs=(vmem, vmem, vmem, vmem),
        scratch_shapes=[
            pltpu.VMEM(main_query.shape, bf16),
            pltpu.VMEM((flat_rows, index_width), bf16),
            pltpu.VMEM((flat_rows // 2, early), bf16),
            pltpu.VMEM((flat_rows // 2, length), bf16),
            pltpu.VMEM((ctx_count,) + latent_key.shape, bf16),
            pltpu.VMEM((ctx_count,) + index_key.shape, bf16),
            pltpu.VMEM((width + 2 * HALF, length), bf16),
            pltpu.VMEM((index_width, length), bf16),
            pltpu.VMEM((index_width, flat_rows), bf16),
            pltpu.VMEM((flat_rows, LANES), f32),
            pltpu.VMEM((flat_rows // 2, early), f32),
            pltpu.VMEM((flat_rows // 2, length), f32),
            pltpu.VMEM((block_rows, packed), f32),
            pltpu.VMEM((block_rows, packed), f32),
            pltpu.VMEM((head_axis, quarter, packed), f32),
            pltpu.VMEM((head_axis, quarter, packed), f32),
            pltpu.VMEM((block_rows, packed), bf16),
            pltpu.VMEM((head_axis, 2, quarter, LANES), f32),
            pltpu.VMEM((local_rows, LANES), f32),
            pltpu.VMEM((index_width, length), f32),
            pltpu.VMEM((head_axis, pairs, slot_rows, index_width), f32),
            pltpu.VMEM((head_axis, pairs, slot_rows, index_width), f32),
            pltpu.VMEM((pairs, slot_rows, index_width), f32),
            pltpu.VMEM((ctx_count, slot_rows, index_width), f32),
            pltpu.VMEM((ctx_count, slot_rows, index_width), f32),
            dma,
            dma((3,)),
            dma((4, ctx_count)),
            dma((4, ctx_count)),
            dma((4, ctx_count)),
            dma((4, ctx_count)),
        ]
        + [dma((head_axis,))] * 10
        + [dma((ctx_count,))] * 2,
        compiler_params=pltpu.CompilerParams(
            collective_id=0, has_side_effects=True, vmem_limit_bytes=60 * 1024 * 1024
        ),
    )(
        block_order,
        main_query,
        latent_key,
        index_query.reshape(flat_rows, index_width),
        index_weight.T,
        index_key,
    )
    loss, grad_rows, grad_weight, grad_key = pl.pallas_call(
        hand_over,
        out_shape=tuple(jax.ShapeDtypeStruct(result.shape, result.dtype) for result in results),
        in_specs=[vmem] * len(results),
        out_specs=(vmem,) * len(results),
    )(*results)
    return (
        loss.reshape(local_rows),
        grad_rows.reshape(local_rows, index_heads, index_width),
        grad_weight.T,
        grad_key,
    )


def solution(mesh):
    in_specs = (
        P(),
        P("ctx", "head"),
        P(None, "ctx"),
        P("ctx", "head", None),
        P("ctx", "head"),
        P(None, "ctx"),
    )
    out_specs = (P("ctx"), P("ctx", "head", None), P("ctx", "head"), P(("ctx", "head"), None))
    return jax.shard_map(body, mesh=mesh, in_specs=in_specs, out_specs=out_specs, check_vma=False)
```

```python
import functools
import math

import jax
import jax.numpy as jnp
from jax import lax
from jax.experimental import pallas as pl
from jax.experimental.pallas import tpu as pltpu
from jax.sharding import PartitionSpec as P

HEAD_QK = 192
LANES = 128
HALF = 64
masked_value = -1e30


def each(lower, upper, step):
    if upper - lower <= 16:
        for index in range(lower, upper):
            step(index)
    else:
        lax.fori_loop(lower, upper, lambda index, carry: (step(index), carry)[1], 0)


def total_over(upper, term):
    if upper <= 16:
        return functools.reduce(lambda a, b: a + b, [term(index) for index in range(upper)])
    return lax.fori_loop(0, upper, lambda index, carry: carry + term(index), jnp.int32(0))


def dot(a, b):
    return jnp.dot(a, b, preferred_element_type=jnp.float32)


def kernel(
    dims,
    order_ref,
    query_ref,
    latent_in,
    rows_in,
    weight_ref,
    index_in,
    loss_ref,
    grad_rows_ref,
    grad_weight_ref,
    grad_key_ref,
    query_vmem,
    rows_ref,
    through_early,
    through_late,
    all_latent,
    all_index,
    window_latent,
    window_index,
    rows_turned,
    weight_col,
    act_early,
    act_late,
    part_logit,
    part_target,
    got_logit,
    got_target,
    slopes,
    losses,
    weight_grads,
    key_turned,
    key_parts,
    got_key,
    key_piece,
    key_send,
    got_piece,
    query_sem,
    input_sem,
    index_send,
    index_recv,
    latent_send,
    latent_recv,
    logit_send,
    logit_recv,
    target_send,
    target_recv,
    slope_send,
    slope_recv,
    loss_send,
    loss_recv,
    key_send_sem,
    key_recv_sem,
    piece_send,
    piece_recv,
):
    ctx_count, head_axis, block_rows, heads, width, index_heads = dims
    pairs = ctx_count // 2
    length = ctx_count * block_rows
    early = length // 2
    quarter = block_rows // head_axis
    me = lax.axis_index("ctx")
    head = lax.axis_index("head")
    across = (head + 2) % 4
    beside = head + 1 - 2 * (head % 2)

    fetch_query = pltpu.make_async_copy(query_ref, query_vmem, query_sem)
    fetch_inputs = [
        pltpu.make_async_copy(index_in, all_index.at[me], input_sem.at[0]),
        pltpu.make_async_copy(latent_in, all_latent.at[me], input_sem.at[1]),
        pltpu.make_async_copy(rows_in, rows_ref, input_sem.at[2]),
    ]
    for fetch in fetch_inputs:
        fetch.start()
    fetch_query.start()

    barrier = pltpu.get_barrier_semaphore()

    def greet_ctx(offset):
        pl.semaphore_signal(
            barrier, inc=1, device_id={"ctx": (me + offset) % ctx_count}, device_id_type=pl.DeviceIdType.MESH
        )

    def greet_head(offset):
        pl.semaphore_signal(
            barrier, inc=1, device_id={"head": (head + offset) % head_axis}, device_id_type=pl.DeviceIdType.MESH
        )

    each(1, ctx_count, greet_ctx)
    each(1, head_axis, greet_head)
    pl.semaphore_wait(barrier, ctx_count - 1 + head_axis - 1)

    def send(source, target, send_sem, recv_sem, where):
        return pltpu.make_async_remote_copy(
            src_ref=source,
            dst_ref=target,
            send_sem=send_sem,
            recv_sem=recv_sem,
            device_id=where,
            device_id_type=pl.DeviceIdType.MESH,
        )

    def keys_plan(all_ref, sends, recvs):
        depth = all_ref.shape[1] // head_axis

        def piece(owner, quarter_index):
            return all_ref.at[owner, pl.ds(pl.multiple_of(quarter_index * depth, 16), depth), :]

        def first(offset):
            where = {"ctx": (me + offset) % ctx_count}
            return send(piece(me, head), piece(me, head), sends.at[0, offset], recvs.at[0, offset], where)

        def onward(stage, offset):
            owner = (me + ctx_count - offset) % ctx_count
            which = across if stage == 3 else head
            where = {"head": across} if stage == 1 else {"head": beside}
            return send(
                piece(owner, which), piece(owner, which), sends.at[stage, offset], recvs.at[stage, offset], where
            )

        return first, onward

    index_first, index_onward = keys_plan(all_index, index_send, index_recv)
    latent_first, latent_onward = keys_plan(all_latent, latent_send, latent_recv)
    fetch_inputs[0].wait()
    each(1, ctx_count, lambda k: index_first(k).start())
    fetch_inputs[1].wait()
    each(1, ctx_count, lambda k: latent_first(k).start())
    fetch_inputs[2].wait()

    sequence = order_ref[2 * me] // ctx_count
    inner = order_ref[2 * me] % ctx_count

    def holder(pair):
        wanted = sequence * ctx_count + pair
        found = total_over(
            ctx_count, lambda d: jnp.where(order_ref[2 * d] == wanted, jnp.int32(1), jnp.int32(0)) * d
        )
        return jnp.minimum(found, ctx_count - 1)

    flat_rows = 2 * block_rows * index_heads
    rows_turned[...] = rows_ref[...].T
    spread = (
        lax.broadcasted_iota(jnp.int32, (flat_rows, 2 * block_rows), 0) // index_heads
        == lax.broadcasted_iota(jnp.int32, (flat_rows, 2 * block_rows), 1)
    ).astype(jnp.bfloat16)
    spread_weight = lax.dot_general(
        spread, weight_ref[...], (((1,), (1,)), ((), ())), preferred_element_type=jnp.float32
    )
    own_lane = lax.broadcasted_iota(
        jnp.int32, (flat_rows, index_heads), 0
    ) % index_heads == lax.broadcasted_iota(jnp.int32, (flat_rows, index_heads), 1)
    weight_col[...] = jnp.broadcast_to(
        jnp.sum(jnp.where(own_lane, spread_weight, 0.0), axis=1, keepdims=True), (flat_rows, LANES)
    )
    window_latent[0:HALF, :] = jnp.zeros((HALF, length), jnp.bfloat16)
    window_latent[HALF + width :, :] = jnp.zeros((HALF, length), jnp.bfloat16)

    def pass_first(onward, offset):
        onward(0, offset).wait_recv()
        onward(1, offset).start()
        onward(2, offset).start()

    def pass_second(onward, offset):
        onward(1, offset).wait_recv()
        onward(3, offset).start()

    def take_last(onward, offset):
        onward(2, offset).wait_recv()
        onward(3, offset).wait_recv()

    def arrange(all_ref, window_ref, top, depth):
        for pair in range(0, pairs, 2):
            a = all_ref[holder(pair)]
            b = all_ref[holder(pair + 1)]
            low = pair * block_rows
            high = length - (pair + 2) * block_rows
            window_ref[top : top + depth, low : low + LANES] = jnp.concatenate([a[:, :HALF], b[:, :HALF]], axis=1)
            window_ref[top : top + depth, high : high + LANES] = jnp.concatenate([b[:, HALF:], a[:, HALF:]], axis=1)

    chunk_rows = 16
    flat = chunk_rows * index_heads
    chunks = block_rows // chunk_rows
    sides = ((0, early, 0, act_early, through_early), (1, length, early, act_late, through_late))

    def logits_of():
        for side, columns, column_at, act_ref, unused in sides:

            def chunk(i, carry):
                local = pl.multiple_of(i * flat, flat)
                at = pl.multiple_of(side * block_rows * index_heads + i * flat, flat)
                act = dot(rows_ref[pl.ds(at, flat), :], window_index[:, 0:columns])
                act_ref[pl.ds(local, flat), :] = act
                scaled = jnp.maximum(act, 0.0) * weight_col[pl.ds(at, flat), 0:1]
                part_logit[pl.ds(pl.multiple_of(i * chunk_rows, chunk_rows), chunk_rows), column_at : column_at + columns] = (
                    jnp.sum(scaled.reshape(chunk_rows, index_heads, columns), axis=1)
                )
                return carry

            lax.fori_loop(0, chunks, chunk, 0)

    def visible_of(side, rows, row_at, columns):
        block = jnp.where(side == 0, inner, ctx_count - 1 - inner)
        row_pos = block * block_rows + row_at + lax.broadcasted_iota(jnp.int32, (rows, columns), 0)
        return lax.broadcasted_iota(jnp.int32, (rows, columns), 1) <= row_pos

    def share(part_ref, got_ref, sends, recvs, offset):
        peer = (head + offset) % head_axis
        return send(
            part_ref.at[pl.ds(pl.multiple_of(peer * quarter, quarter), quarter), :],
            got_ref.at[offset],
            sends.at[offset],
            recvs.at[offset],
            {"head": peer},
        )

    score_scale = 1.0 / math.sqrt(HEAD_QK)
    group = max(1, min(heads // 2, 2048 // length))
    groups = heads // 2 // group
    padded = width + HALF

    def attention():
        part_target[...] = jnp.zeros(part_target.shape, jnp.float32)
        for parity in range(2):
            top = HALF if parity == 0 else 0
            lane_at = 0 if parity == 0 else width - HALF
            for side, columns, column_at, unused, unused in sides:
                visible = visible_of(side, block_rows, 0, columns)

                def run(i, carry):
                    stacked = jnp.concatenate(
                        [
                            query_vmem[
                                side * block_rows : (side + 1) * block_rows,
                                pl.ds(pl.multiple_of((i * group + g) * 2 * width + lane_at, LANES), padded),
                            ]
                            for g in range(group)
                        ],
                        axis=0,
                    )
                    scores = dot(stacked, window_latent[top : top + padded, 0:columns]) * score_scale
                    total = part_target[:, column_at : column_at + columns]
                    for g in range(group):
                        one = jnp.where(visible, scores[g * block_rows : (g + 1) * block_rows], masked_value)
                        raised = jnp.exp(one - jnp.max(one, axis=1, keepdims=True))
                        total = total + raised * (1.0 / jnp.sum(raised, axis=1, keepdims=True))
                    part_target[:, column_at : column_at + columns] = total
                    return carry

                lax.fori_loop(0, groups, run, 0)

    each(1, ctx_count, lambda k: pass_first(index_onward, k))
    lag = min(3, ctx_count - 1)
    each(1, 1 + lag, lambda k: pass_first(latent_onward, k))
    each(1, ctx_count, lambda k: pass_second(index_onward, k))

    def pass_both(offset):
        pass_first(latent_onward, offset)
        pass_second(latent_onward, offset - lag)

    each(1 + lag, ctx_count, pass_both)
    each(1, ctx_count, lambda k: take_last(index_onward, k))
    arrange(all_index, window_index, 0, window_index.shape[0])
    logits_of()
    each(1, head_axis, lambda k: share(part_logit, got_logit, logit_send, logit_recv, k).start())
    each(ctx_count - lag, ctx_count, lambda k: pass_second(latent_onward, k))
    each(1, ctx_count, lambda k: take_last(latent_onward, k))
    arrange(all_latent, window_latent, HALF, width)
    fetch_query.wait()
    attention()
    each(1, head_axis, lambda k: share(part_target, got_target, target_send, target_recv, k).start())
    each(1, head_axis, lambda k: share(part_logit, got_logit, logit_send, logit_recv, k).wait_recv())
    each(1, head_axis, lambda k: share(part_target, got_target, target_send, target_recv, k).wait_recv())

    my_rows = pl.ds(pl.multiple_of(head * quarter, quarter), quarter)
    for side, columns, column_at, unused, unused in sides:
        at = slice(column_at, column_at + columns)
        visible = visible_of(side, quarter, head * quarter, columns)
        logit = part_logit[my_rows, at]
        target = part_target[my_rows, at]
        for k in range(1, head_axis):
            logit = logit + got_logit[k, :, at]
            target = target + got_target[k, :, at]
        target = target * (1.0 / (heads * head_axis))
        masked = jnp.where(visible, logit, masked_value)
        top = jnp.max(masked, axis=1, keepdims=True)
        lse = top + jnp.log(jnp.sum(jnp.exp(masked - top), axis=1, keepdims=True))
        loss = jnp.sum(jnp.where(visible, target * (lse - logit), 0.0), axis=1, keepdims=True)
        slopes[my_rows, at] = jnp.where(visible, jnp.exp(masked - lse) - target, 0.0).astype(jnp.bfloat16)
        losses[head, side] = jnp.broadcast_to(loss, (quarter, LANES))

    def spread_slopes(offset):
        return send(
            slopes.at[my_rows, :],
            slopes.at[my_rows, :],
            slope_send.at[offset],
            slope_recv.at[offset],
            {"head": (head + offset) % head_axis},
        )

    def spread_losses(offset):
        return send(
            losses.at[head],
            losses.at[head],
            loss_send.at[offset],
            loss_recv.at[offset],
            {"head": (head + offset) % head_axis},
        )

    each(1, head_axis, lambda k: spread_slopes(k).start())
    each(1, head_axis, lambda k: spread_losses(k).start())
    each(1, head_axis, lambda k: spread_slopes(k).wait_recv())

    key_turned[...] = jnp.zeros(key_turned.shape, jnp.float32)
    lane_of = lax.broadcasted_iota(jnp.int32, (flat, LANES), 1)
    lane_own = lane_of == lax.broadcasted_iota(jnp.int32, (flat, LANES), 0) % index_heads
    def slope_of(rows_at, column_at, columns):
        slope = slopes[pl.ds(rows_at, chunk_rows), column_at : column_at + columns].astype(jnp.float32)
        return jnp.broadcast_to(slope[:, None, :], (chunk_rows, index_heads, columns)).reshape(flat, columns)

    for side, columns, column_at, act_ref, through_ref in sides:

        def chunk(i, carry):
            local = pl.multiple_of(i * flat, flat)
            at = pl.multiple_of(side * block_rows * index_heads + i * flat, flat)
            rows_at = pl.multiple_of(i * chunk_rows, chunk_rows)
            act = act_ref[pl.ds(local, flat), :]
            slope = slope_of(rows_at, column_at, columns)
            through = jnp.where(act > 0.0, slope * weight_col[pl.ds(at, flat), 0:1], 0.0).astype(jnp.bfloat16)
            through_ref[pl.ds(local, flat), :] = through
            key_turned[:, 0:columns] += dot(rows_turned[:, pl.ds(at, flat)], through)
            return carry

        lax.fori_loop(0, chunks, chunk, 0)

    def row_grads():
        for side, columns, column_at, act_ref, through_ref in sides:

            def chunk(i, carry):
                local = pl.multiple_of(i * flat, flat)
                at = pl.multiple_of(side * block_rows * index_heads + i * flat, flat)
                rows_at = pl.multiple_of(i * chunk_rows, chunk_rows)
                slope = slope_of(rows_at, column_at, columns)
                col = jnp.sum(slope * jnp.maximum(act_ref[pl.ds(local, flat), :], 0.0), axis=1, keepdims=True)
                placed = jnp.where(lane_own, col, 0.0).reshape(chunk_rows, index_heads, LANES)
                weight_at = pl.multiple_of(side * block_rows + i * chunk_rows, chunk_rows)
                weight_grads[pl.ds(weight_at, chunk_rows), :] = jnp.sum(placed, axis=1)
                grad_rows_ref[pl.ds(at, flat), :] = lax.dot_general(
                    through_ref[pl.ds(local, flat), :],
                    window_index[:, 0:columns],
                    (((1,), (1,)), ((), ())),
                    preferred_element_type=jnp.float32,
                ).astype(jnp.bfloat16)
                return carry

            lax.fori_loop(0, chunks, chunk, 0)
        grad_weight_ref[...] = weight_grads[...].T[0:index_heads].astype(jnp.bfloat16)

    slot_rows = 2 * block_rows // head_axis
    for pair in range(pairs):
        low = pair * block_rows
        high = length - (pair + 1) * block_rows
        for part, start in ((0, low), (2, high)):
            lanes_at = start // LANES * LANES
            turned = key_turned[:, lanes_at : lanes_at + LANES].T
            for k in range(2):
                begin = start - lanes_at + k * slot_rows
                key_parts[part + k, pair] = turned[begin : begin + slot_rows].astype(jnp.bfloat16)

    def share_key(offset):
        peer = (head + offset) % head_axis
        return send(
            key_parts.at[peer], got_key.at[offset], key_send_sem.at[offset], key_recv_sem.at[offset], {"head": peer}
        )

    each(1, head_axis, lambda k: share_key(k).start())
    row_grads()
    each(1, head_axis, lambda k: spread_losses(k).wait_recv())
    loss_block = jnp.concatenate(
        [losses[q, side] for side in range(2) for q in range(head_axis)], axis=0
    )
    diagonal = lax.broadcasted_iota(jnp.int32, loss_block.shape, 0) == lax.broadcasted_iota(
        jnp.int32, loss_block.shape, 1
    )
    loss_ref[...] = jnp.sum(jnp.where(diagonal, loss_block, 0.0), axis=0, keepdims=True)
    each(1, head_axis, lambda k: share_key(k).wait_recv())
    for pair in range(pairs):
        piece = key_parts[head, pair].astype(jnp.float32)
        for k in range(1, head_axis):
            piece = piece + got_key[k, pair].astype(jnp.float32)
        key_piece[pair] = piece

    def fill(d):
        block = order_ref[2 * d]
        same = block // ctx_count == sequence
        key_send[d] = jnp.where(same, key_piece[block % ctx_count], 0.0).astype(jnp.bfloat16)

    each(0, ctx_count, fill)

    def share_piece(offset):
        peer = (me + offset) % ctx_count
        return send(
            key_send.at[peer], got_piece.at[offset], piece_send.at[offset], piece_recv.at[offset], {"ctx": peer}
        )

    each(1, ctx_count, lambda k: share_piece(k).start())
    grad_key_ref[...] = key_piece[inner]

    def add(offset):
        share_piece(offset).wait_recv()
        grad_key_ref[...] += got_piece[offset].astype(jnp.float32)

    each(1, ctx_count, add)

    def finish_ctx(offset):
        index_first(offset).wait_send()
        latent_first(offset).wait_send()
        for stage in range(1, 4):
            index_onward(stage, offset).wait_send()
            latent_onward(stage, offset).wait_send()
        share_piece(offset).wait_send()

    def finish_head(offset):
        share(part_logit, got_logit, logit_send, logit_recv, offset).wait_send()
        share(part_target, got_target, target_send, target_recv, offset).wait_send()
        spread_slopes(offset).wait_send()
        spread_losses(offset).wait_send()
        share_key(offset).wait_send()

    each(1, ctx_count, finish_ctx)
    each(1, head_axis, finish_head)


def hand_over(*refs):
    count = len(refs) // 2
    for source, target in zip(refs[:count], refs[count:]):
        target[...] = source[...]


def body(block_order, main_query, latent_key, index_query, index_weight, index_key):
    ctx_count = lax.axis_size("ctx")
    head_axis = lax.axis_size("head")
    local_rows = main_query.shape[0]
    block_rows = local_rows // 2
    width = latent_key.shape[0]
    heads = main_query.shape[1] // width
    index_heads, index_width = index_query.shape[1:]
    length = ctx_count * block_rows
    early = length // 2
    packed = early + length
    pairs = ctx_count // 2
    quarter = block_rows // head_axis
    slot_rows = local_rows // head_axis
    flat_rows = local_rows * index_heads
    f32, bf16 = jnp.float32, jnp.bfloat16
    vmem = pl.BlockSpec(memory_space=pltpu.VMEM)
    hbm = pl.BlockSpec(memory_space=pl.ANY)
    dma = pltpu.SemaphoreType.DMA
    results = pl.pallas_call(
        functools.partial(kernel, (ctx_count, head_axis, block_rows, heads, width, index_heads)),
        out_shape=(
            jax.ShapeDtypeStruct((1, local_rows), f32),
            jax.ShapeDtypeStruct((flat_rows, index_width), bf16),
            jax.ShapeDtypeStruct((index_heads, local_rows), bf16),
            jax.ShapeDtypeStruct((slot_rows, index_width), f32),
        ),
        in_specs=[
            pl.BlockSpec(memory_space=pltpu.SMEM),
            hbm,
            hbm,
            hbm,
            vmem,
            hbm,
        ],
        out_specs=(vmem, vmem, vmem, vmem),
        scratch_shapes=[
            pltpu.VMEM(main_query.shape, bf16),
            pltpu.VMEM((flat_rows, index_width), bf16),
            pltpu.VMEM((flat_rows // 2, early), bf16),
            pltpu.VMEM((flat_rows // 2, length), bf16),
            pltpu.VMEM((ctx_count,) + latent_key.shape, bf16),
            pltpu.VMEM((ctx_count,) + index_key.shape, bf16),
            pltpu.VMEM((width + 2 * HALF, length), bf16),
            pltpu.VMEM((index_width, length), bf16),
            pltpu.VMEM((index_width, flat_rows), bf16),
            pltpu.VMEM((flat_rows, LANES), f32),
            pltpu.VMEM((flat_rows // 2, early), f32),
            pltpu.VMEM((flat_rows // 2, length), f32),
            pltpu.VMEM((block_rows, packed), f32),
            pltpu.VMEM((block_rows, packed), f32),
            pltpu.VMEM((head_axis, quarter, packed), f32),
            pltpu.VMEM((head_axis, quarter, packed), f32),
            pltpu.VMEM((block_rows, packed), bf16),
            pltpu.VMEM((head_axis, 2, quarter, LANES), f32),
            pltpu.VMEM((local_rows, LANES), f32),
            pltpu.VMEM((index_width, length), f32),
            pltpu.VMEM((head_axis, pairs, slot_rows, index_width), bf16),
            pltpu.VMEM((head_axis, pairs, slot_rows, index_width), bf16),
            pltpu.VMEM((pairs, slot_rows, index_width), f32),
            pltpu.VMEM((ctx_count, slot_rows, index_width), bf16),
            pltpu.VMEM((ctx_count, slot_rows, index_width), bf16),
            dma,
            dma((3,)),
            dma((4, ctx_count)),
            dma((4, ctx_count)),
            dma((4, ctx_count)),
            dma((4, ctx_count)),
        ]
        + [dma((head_axis,))] * 10
        + [dma((ctx_count,))] * 2,
        compiler_params=pltpu.CompilerParams(
            collective_id=0, has_side_effects=True, vmem_limit_bytes=60 * 1024 * 1024
        ),
    )(
        block_order,
        main_query,
        latent_key,
        index_query.reshape(flat_rows, index_width),
        index_weight.T,
        index_key,
    )
    loss, grad_rows, grad_weight, grad_key = pl.pallas_call(
        hand_over,
        out_shape=tuple(jax.ShapeDtypeStruct(result.shape, result.dtype) for result in results),
        in_specs=[vmem] * len(results),
        out_specs=(vmem,) * len(results),
    )(*results)
    return (
        loss.reshape(local_rows),
        grad_rows.reshape(local_rows, index_heads, index_width),
        grad_weight.T,
        grad_key,
    )


def solution(mesh):
    in_specs = (
        P(),
        P("ctx", "head"),
        P(None, "ctx"),
        P("ctx", "head", None),
        P("ctx", "head"),
        P(None, "ctx"),
    )
    out_specs = (P("ctx"), P("ctx", "head", None), P("ctx", "head"), P(("ctx", "head"), None))
    return jax.shard_map(body, mesh=mesh, in_specs=in_specs, out_specs=out_specs, check_vma=False)
```

```python
import functools
import math

import jax
import jax.numpy as jnp
from jax import lax
from jax.experimental import pallas as pl
from jax.experimental.pallas import tpu as pltpu
from jax.sharding import PartitionSpec as P

HEAD_QK = 192
LANES = 128
HALF = 64
masked_value = -1e30


def each(lower, upper, step):
    if upper - lower <= 16:
        for index in range(lower, upper):
            step(index)
    else:
        lax.fori_loop(lower, upper, lambda index, carry: (step(index), carry)[1], 0)


def total_over(upper, term):
    if upper <= 16:
        return functools.reduce(lambda a, b: a + b, [term(index) for index in range(upper)])
    return lax.fori_loop(0, upper, lambda index, carry: carry + term(index), jnp.int32(0))


def dot(a, b):
    return jnp.dot(a, b, preferred_element_type=jnp.float32)


def kernel(
    dims,
    order_ref,
    query_ref,
    latent_in,
    rows_in,
    weight_ref,
    index_in,
    loss_ref,
    grad_rows_ref,
    grad_weight_ref,
    grad_key_ref,
    query_vmem,
    rows_ref,
    through_early,
    through_late,
    all_latent,
    all_index,
    window_latent,
    window_index,
    rows_turned,
    weight_col,
    act_early,
    act_late,
    part_logit,
    part_target,
    got_logit,
    got_target,
    slopes,
    losses,
    weight_grads,
    key_turned,
    key_parts,
    got_key,
    key_piece,
    key_send,
    got_piece,
    query_sem,
    input_sem,
    index_send,
    index_recv,
    latent_send,
    latent_recv,
    logit_send,
    logit_recv,
    target_send,
    target_recv,
    slope_send,
    slope_recv,
    loss_send,
    loss_recv,
    key_send_sem,
    key_recv_sem,
    piece_send,
    piece_recv,
):
    ctx_count, head_axis, block_rows, heads, width, index_heads = dims
    pairs = ctx_count // 2
    length = ctx_count * block_rows
    early = length // 2
    quarter = block_rows // head_axis
    me = lax.axis_index("ctx")
    head = lax.axis_index("head")
    across = (head + 2) % 4
    beside = head + 1 - 2 * (head % 2)

    fetch_query = pltpu.make_async_copy(query_ref, query_vmem, query_sem)
    fetch_inputs = [
        pltpu.make_async_copy(index_in, all_index.at[me], input_sem.at[0]),
        pltpu.make_async_copy(latent_in, all_latent.at[me], input_sem.at[1]),
        pltpu.make_async_copy(rows_in, rows_ref, input_sem.at[2]),
    ]
    for fetch in fetch_inputs:
        fetch.start()
    fetch_query.start()

    barrier = pltpu.get_barrier_semaphore()

    def greet_ctx(offset):
        pl.semaphore_signal(
            barrier, inc=1, device_id={"ctx": (me + offset) % ctx_count}, device_id_type=pl.DeviceIdType.MESH
        )

    def greet_head(offset):
        pl.semaphore_signal(
            barrier, inc=1, device_id={"head": (head + offset) % head_axis}, device_id_type=pl.DeviceIdType.MESH
        )

    each(1, ctx_count, greet_ctx)
    each(1, head_axis, greet_head)
    pl.semaphore_wait(barrier, ctx_count - 1 + head_axis - 1)

    def send(source, target, send_sem, recv_sem, where):
        return pltpu.make_async_remote_copy(
            src_ref=source,
            dst_ref=target,
            send_sem=send_sem,
            recv_sem=recv_sem,
            device_id=where,
            device_id_type=pl.DeviceIdType.MESH,
        )

    def keys_plan(all_ref, sends, recvs):
        depth = all_ref.shape[1] // head_axis

        def piece(owner, quarter_index):
            return all_ref.at[owner, pl.ds(pl.multiple_of(quarter_index * depth, 16), depth), :]

        def first(offset):
            where = {"ctx": (me + offset) % ctx_count}
            return send(piece(me, head), piece(me, head), sends.at[0, offset], recvs.at[0, offset], where)

        def onward(stage, offset):
            owner = (me + ctx_count - offset) % ctx_count
            which = across if stage == 3 else head
            where = {"head": across} if stage == 1 else {"head": beside}
            return send(
                piece(owner, which), piece(owner, which), sends.at[stage, offset], recvs.at[stage, offset], where
            )

        return first, onward

    index_first, index_onward = keys_plan(all_index, index_send, index_recv)
    latent_first, latent_onward = keys_plan(all_latent, latent_send, latent_recv)
    fetch_inputs[0].wait()
    each(1, ctx_count, lambda k: index_first(k).start())
    fetch_inputs[1].wait()
    each(1, ctx_count, lambda k: latent_first(k).start())
    fetch_inputs[2].wait()

    sequence = order_ref[2 * me] // ctx_count
    inner = order_ref[2 * me] % ctx_count

    def holder(pair):
        wanted = sequence * ctx_count + pair
        found = total_over(
            ctx_count, lambda d: jnp.where(order_ref[2 * d] == wanted, jnp.int32(1), jnp.int32(0)) * d
        )
        return jnp.minimum(found, ctx_count - 1)

    flat_rows = 2 * block_rows * index_heads
    rows_turned[...] = rows_ref[...].T
    spread = (
        lax.broadcasted_iota(jnp.int32, (flat_rows, 2 * block_rows), 0) // index_heads
        == lax.broadcasted_iota(jnp.int32, (flat_rows, 2 * block_rows), 1)
    ).astype(jnp.bfloat16)
    spread_weight = lax.dot_general(
        spread, weight_ref[...], (((1,), (1,)), ((), ())), preferred_element_type=jnp.float32
    )
    own_lane = lax.broadcasted_iota(
        jnp.int32, (flat_rows, index_heads), 0
    ) % index_heads == lax.broadcasted_iota(jnp.int32, (flat_rows, index_heads), 1)
    weight_col[...] = jnp.broadcast_to(
        jnp.sum(jnp.where(own_lane, spread_weight, 0.0), axis=1, keepdims=True), (flat_rows, LANES)
    )
    window_latent[0:HALF, :] = jnp.zeros((HALF, length), jnp.bfloat16)
    window_latent[HALF + width :, :] = jnp.zeros((HALF, length), jnp.bfloat16)

    def pass_first(onward, offset):
        onward(0, offset).wait_recv()
        onward(1, offset).start()
        onward(2, offset).start()

    def pass_second(onward, offset):
        onward(1, offset).wait_recv()
        onward(3, offset).start()

    def take_last(onward, offset):
        onward(2, offset).wait_recv()
        onward(3, offset).wait_recv()

    def arrange(all_ref, window_ref, top, depth):
        for pair in range(0, pairs, 2):
            a = all_ref[holder(pair)]
            b = all_ref[holder(pair + 1)]
            low = pair * block_rows
            high = length - (pair + 2) * block_rows
            window_ref[top : top + depth, low : low + LANES] = jnp.concatenate([a[:, :HALF], b[:, :HALF]], axis=1)
            window_ref[top : top + depth, high : high + LANES] = jnp.concatenate([b[:, HALF:], a[:, HALF:]], axis=1)

    chunk_rows = 16
    flat = chunk_rows * index_heads
    chunks = block_rows // chunk_rows
    sides = ((0, early, 0, act_early, through_early), (1, length, early, act_late, through_late))

    def logits_of():
        for side, columns, column_at, act_ref, unused in sides:

            def chunk(i, carry):
                local = pl.multiple_of(i * flat, flat)
                at = pl.multiple_of(side * block_rows * index_heads + i * flat, flat)
                act = dot(rows_ref[pl.ds(at, flat), :], window_index[:, 0:columns])
                act_ref[pl.ds(local, flat), :] = act
                scaled = jnp.maximum(act, 0.0) * weight_col[pl.ds(at, flat), 0:1]
                part_logit[pl.ds(pl.multiple_of(i * chunk_rows, chunk_rows), chunk_rows), column_at : column_at + columns] = (
                    jnp.sum(scaled.reshape(chunk_rows, index_heads, columns), axis=1)
                )
                return carry

            lax.fori_loop(0, chunks, chunk, 0)

    def visible_of(side, rows, row_at, columns):
        block = jnp.where(side == 0, inner, ctx_count - 1 - inner)
        row_pos = block * block_rows + row_at + lax.broadcasted_iota(jnp.int32, (rows, columns), 0)
        return lax.broadcasted_iota(jnp.int32, (rows, columns), 1) <= row_pos

    def share(part_ref, got_ref, sends, recvs, offset):
        peer = (head + offset) % head_axis
        return send(
            part_ref.at[pl.ds(pl.multiple_of(peer * quarter, quarter), quarter), :],
            got_ref.at[offset],
            sends.at[offset],
            recvs.at[offset],
            {"head": peer},
        )

    score_scale = 1.0 / math.sqrt(HEAD_QK)
    group = max(1, min(heads // 2, 2048 // length))
    groups = heads // 2 // group
    padded = width + HALF

    def attention():
        part_target[...] = jnp.zeros(part_target.shape, jnp.float32)
        for parity in range(2):
            top = HALF if parity == 0 else 0
            lane_at = 0 if parity == 0 else width - HALF
            for side, columns, column_at, unused, unused in sides:
                visible = visible_of(side, block_rows, 0, columns)

                def run(i, carry):
                    stacked = jnp.concatenate(
                        [
                            query_vmem[
                                side * block_rows : (side + 1) * block_rows,
                                pl.ds(pl.multiple_of((i * group + g) * 2 * width + lane_at, LANES), padded),
                            ]
                            for g in range(group)
                        ],
                        axis=0,
                    )
                    scores = dot(stacked, window_latent[top : top + padded, 0:columns]) * score_scale
                    total = part_target[:, column_at : column_at + columns]
                    for g in range(group):
                        one = jnp.where(visible, scores[g * block_rows : (g + 1) * block_rows], masked_value)
                        raised = jnp.exp(one - jnp.max(one, axis=1, keepdims=True))
                        total = total + raised * (1.0 / jnp.sum(raised, axis=1, keepdims=True))
                    part_target[:, column_at : column_at + columns] = total
                    return carry

                lax.fori_loop(0, groups, run, 0)

    each(1, ctx_count, lambda k: pass_first(index_onward, k))
    each(1, ctx_count, lambda k: pass_first(latent_onward, k))
    each(1, ctx_count, lambda k: pass_second(index_onward, k))
    each(1, ctx_count, lambda k: take_last(index_onward, k))
    arrange(all_index, window_index, 0, window_index.shape[0])
    logits_of()
    each(1, head_axis, lambda k: share(part_logit, got_logit, logit_send, logit_recv, k).start())
    each(1, ctx_count, lambda k: pass_second(latent_onward, k))
    each(1, ctx_count, lambda k: take_last(latent_onward, k))
    arrange(all_latent, window_latent, HALF, width)
    fetch_query.wait()
    attention()
    each(1, head_axis, lambda k: share(part_target, got_target, target_send, target_recv, k).start())
    each(1, head_axis, lambda k: share(part_logit, got_logit, logit_send, logit_recv, k).wait_recv())
    each(1, head_axis, lambda k: share(part_target, got_target, target_send, target_recv, k).wait_recv())

    my_rows = pl.ds(pl.multiple_of(head * quarter, quarter), quarter)
    for side, columns, column_at, unused, unused in sides:
        at = slice(column_at, column_at + columns)
        visible = visible_of(side, quarter, head * quarter, columns)
        logit = part_logit[my_rows, at]
        target = part_target[my_rows, at]
        for k in range(1, head_axis):
            logit = logit + got_logit[k, :, at]
            target = target + got_target[k, :, at]
        target = target * (1.0 / (heads * head_axis))
        masked = jnp.where(visible, logit, masked_value)
        top = jnp.max(masked, axis=1, keepdims=True)
        lse = top + jnp.log(jnp.sum(jnp.exp(masked - top), axis=1, keepdims=True))
        loss = jnp.sum(jnp.where(visible, target * (lse - logit), 0.0), axis=1, keepdims=True)
        slopes[my_rows, at] = jnp.where(visible, jnp.exp(masked - lse) - target, 0.0).astype(jnp.bfloat16)
        losses[head, side] = jnp.broadcast_to(loss, (quarter, LANES))

    def spread_slopes(offset):
        return send(
            slopes.at[my_rows, :],
            slopes.at[my_rows, :],
            slope_send.at[offset],
            slope_recv.at[offset],
            {"head": (head + offset) % head_axis},
        )

    def spread_losses(offset):
        return send(
            losses.at[head],
            losses.at[head],
            loss_send.at[offset],
            loss_recv.at[offset],
            {"head": (head + offset) % head_axis},
        )

    each(1, head_axis, lambda k: spread_slopes(k).start())
    each(1, head_axis, lambda k: spread_losses(k).start())
    each(1, head_axis, lambda k: spread_slopes(k).wait_recv())

    key_turned[...] = jnp.zeros(key_turned.shape, jnp.float32)
    lane_of = lax.broadcasted_iota(jnp.int32, (flat, LANES), 1)
    lane_own = lane_of == lax.broadcasted_iota(jnp.int32, (flat, LANES), 0) % index_heads
    def slope_of(rows_at, column_at, columns):
        slope = slopes[pl.ds(rows_at, chunk_rows), column_at : column_at + columns].astype(jnp.float32)
        return jnp.broadcast_to(slope[:, None, :], (chunk_rows, index_heads, columns)).reshape(flat, columns)

    for side, columns, column_at, act_ref, through_ref in sides:

        def chunk(i, carry):
            local = pl.multiple_of(i * flat, flat)
            at = pl.multiple_of(side * block_rows * index_heads + i * flat, flat)
            rows_at = pl.multiple_of(i * chunk_rows, chunk_rows)
            act = act_ref[pl.ds(local, flat), :]
            slope = slope_of(rows_at, column_at, columns)
            through = jnp.where(act > 0.0, slope * weight_col[pl.ds(at, flat), 0:1], 0.0).astype(jnp.bfloat16)
            through_ref[pl.ds(local, flat), :] = through
            key_turned[:, 0:columns] += dot(rows_turned[:, pl.ds(at, flat)], through)
            return carry

        lax.fori_loop(0, chunks, chunk, 0)

    def row_grads():
        for side, columns, column_at, act_ref, through_ref in sides:

            def chunk(i, carry):
                local = pl.multiple_of(i * flat, flat)
                at = pl.multiple_of(side * block_rows * index_heads + i * flat, flat)
                rows_at = pl.multiple_of(i * chunk_rows, chunk_rows)
                slope = slope_of(rows_at, column_at, columns)
                col = jnp.sum(slope * jnp.maximum(act_ref[pl.ds(local, flat), :], 0.0), axis=1, keepdims=True)
                placed = jnp.where(lane_own, col, 0.0).reshape(chunk_rows, index_heads, LANES)
                weight_at = pl.multiple_of(side * block_rows + i * chunk_rows, chunk_rows)
                weight_grads[pl.ds(weight_at, chunk_rows), :] = jnp.sum(placed, axis=1)
                grad_rows_ref[pl.ds(at, flat), :] = lax.dot_general(
                    through_ref[pl.ds(local, flat), :],
                    window_index[:, 0:columns],
                    (((1,), (1,)), ((), ())),
                    preferred_element_type=jnp.float32,
                ).astype(jnp.bfloat16)
                return carry

            lax.fori_loop(0, chunks, chunk, 0)
        grad_weight_ref[...] = weight_grads[...].T[0:index_heads].astype(jnp.bfloat16)

    slot_rows = 2 * block_rows // head_axis
    for pair in range(pairs):
        low = pair * block_rows
        high = length - (pair + 1) * block_rows
        for part, start in ((0, low), (2, high)):
            lanes_at = start // LANES * LANES
            turned = key_turned[:, lanes_at : lanes_at + LANES].T
            for k in range(2):
                begin = start - lanes_at + k * slot_rows
                key_parts[part + k, pair] = turned[begin : begin + slot_rows].astype(jnp.bfloat16)

    def share_key(offset):
        peer = (head + offset) % head_axis
        return send(
            key_parts.at[peer], got_key.at[offset], key_send_sem.at[offset], key_recv_sem.at[offset], {"head": peer}
        )

    each(1, head_axis, lambda k: share_key(k).start())
    row_grads()
    each(1, head_axis, lambda k: spread_losses(k).wait_recv())
    loss_block = jnp.concatenate(
        [losses[q, side] for side in range(2) for q in range(head_axis)], axis=0
    )
    diagonal = lax.broadcasted_iota(jnp.int32, loss_block.shape, 0) == lax.broadcasted_iota(
        jnp.int32, loss_block.shape, 1
    )
    loss_ref[...] = jnp.sum(jnp.where(diagonal, loss_block, 0.0), axis=0, keepdims=True)
    each(1, head_axis, lambda k: share_key(k).wait_recv())
    for pair in range(pairs):
        piece = key_parts[head, pair].astype(jnp.float32)
        for k in range(1, head_axis):
            piece = piece + got_key[k, pair].astype(jnp.float32)
        key_piece[pair] = piece

    def fill(d):
        block = order_ref[2 * d]
        same = block // ctx_count == sequence
        key_send[d] = jnp.where(same, key_piece[block % ctx_count], 0.0).astype(jnp.bfloat16)

    each(0, ctx_count, fill)

    def share_piece(offset):
        peer = (me + offset) % ctx_count
        return send(
            key_send.at[peer], got_piece.at[offset], piece_send.at[offset], piece_recv.at[offset], {"ctx": peer}
        )

    each(1, ctx_count, lambda k: share_piece(k).start())
    grad_key_ref[...] = key_piece[inner]

    def add(offset):
        share_piece(offset).wait_recv()
        grad_key_ref[...] += got_piece[offset].astype(jnp.float32)

    each(1, ctx_count, add)

    def finish_ctx(offset):
        index_first(offset).wait_send()
        latent_first(offset).wait_send()
        for stage in range(1, 4):
            index_onward(stage, offset).wait_send()
            latent_onward(stage, offset).wait_send()
        share_piece(offset).wait_send()

    def finish_head(offset):
        share(part_logit, got_logit, logit_send, logit_recv, offset).wait_send()
        share(part_target, got_target, target_send, target_recv, offset).wait_send()
        spread_slopes(offset).wait_send()
        spread_losses(offset).wait_send()
        share_key(offset).wait_send()

    each(1, ctx_count, finish_ctx)
    each(1, head_axis, finish_head)


def hand_over(*refs):
    count = len(refs) // 2
    for source, target in zip(refs[:count], refs[count:]):
        target[...] = source[...]


def body(block_order, main_query, latent_key, index_query, index_weight, index_key):
    ctx_count = lax.axis_size("ctx")
    head_axis = lax.axis_size("head")
    local_rows = main_query.shape[0]
    block_rows = local_rows // 2
    width = latent_key.shape[0]
    heads = main_query.shape[1] // width
    index_heads, index_width = index_query.shape[1:]
    length = ctx_count * block_rows
    early = length // 2
    packed = early + length
    pairs = ctx_count // 2
    quarter = block_rows // head_axis
    slot_rows = local_rows // head_axis
    flat_rows = local_rows * index_heads
    f32, bf16 = jnp.float32, jnp.bfloat16
    vmem = pl.BlockSpec(memory_space=pltpu.VMEM)
    hbm = pl.BlockSpec(memory_space=pl.ANY)
    dma = pltpu.SemaphoreType.DMA
    results = pl.pallas_call(
        functools.partial(kernel, (ctx_count, head_axis, block_rows, heads, width, index_heads)),
        out_shape=(
            jax.ShapeDtypeStruct((1, local_rows), f32),
            jax.ShapeDtypeStruct((flat_rows, index_width), bf16),
            jax.ShapeDtypeStruct((index_heads, local_rows), bf16),
            jax.ShapeDtypeStruct((slot_rows, index_width), f32),
        ),
        in_specs=[
            pl.BlockSpec(memory_space=pltpu.SMEM),
            hbm,
            hbm,
            hbm,
            vmem,
            hbm,
        ],
        out_specs=(vmem, vmem, vmem, vmem),
        scratch_shapes=[
            pltpu.VMEM(main_query.shape, bf16),
            pltpu.VMEM((flat_rows, index_width), bf16),
            pltpu.VMEM((flat_rows // 2, early), bf16),
            pltpu.VMEM((flat_rows // 2, length), bf16),
            pltpu.VMEM((ctx_count,) + latent_key.shape, bf16),
            pltpu.VMEM((ctx_count,) + index_key.shape, bf16),
            pltpu.VMEM((width + 2 * HALF, length), bf16),
            pltpu.VMEM((index_width, length), bf16),
            pltpu.VMEM((index_width, flat_rows), bf16),
            pltpu.VMEM((flat_rows, LANES), f32),
            pltpu.VMEM((flat_rows // 2, early), f32),
            pltpu.VMEM((flat_rows // 2, length), f32),
            pltpu.VMEM((block_rows, packed), f32),
            pltpu.VMEM((block_rows, packed), f32),
            pltpu.VMEM((head_axis, quarter, packed), f32),
            pltpu.VMEM((head_axis, quarter, packed), f32),
            pltpu.VMEM((block_rows, packed), bf16),
            pltpu.VMEM((head_axis, 2, quarter, LANES), f32),
            pltpu.VMEM((local_rows, LANES), f32),
            pltpu.VMEM((index_width, length), f32),
            pltpu.VMEM((head_axis, pairs, slot_rows, index_width), bf16),
            pltpu.VMEM((head_axis, pairs, slot_rows, index_width), bf16),
            pltpu.VMEM((pairs, slot_rows, index_width), f32),
            pltpu.VMEM((ctx_count, slot_rows, index_width), bf16),
            pltpu.VMEM((ctx_count, slot_rows, index_width), bf16),
            dma,
            dma((3,)),
            dma((4, ctx_count)),
            dma((4, ctx_count)),
            dma((4, ctx_count)),
            dma((4, ctx_count)),
        ]
        + [dma((head_axis,))] * 10
        + [dma((ctx_count,))] * 2,
        compiler_params=pltpu.CompilerParams(
            collective_id=0, has_side_effects=True, vmem_limit_bytes=60 * 1024 * 1024
        ),
    )(
        block_order,
        main_query,
        latent_key,
        index_query.reshape(flat_rows, index_width),
        index_weight.T,
        index_key,
    )
    loss, grad_rows, grad_weight, grad_key = pl.pallas_call(
        hand_over,
        out_shape=tuple(jax.ShapeDtypeStruct(result.shape, result.dtype) for result in results),
        in_specs=[vmem] * len(results),
        out_specs=(vmem,) * len(results),
    )(*results)
    return (
        loss.reshape(local_rows),
        grad_rows.reshape(local_rows, index_heads, index_width),
        grad_weight.T,
        grad_key,
    )


def solution(mesh):
    in_specs = (
        P(),
        P("ctx", "head"),
        P(None, "ctx"),
        P("ctx", "head", None),
        P("ctx", "head"),
        P(None, "ctx"),
    )
    out_specs = (P("ctx"), P("ctx", "head", None), P("ctx", "head"), P(("ctx", "head"), None))
    return jax.shard_map(body, mesh=mesh, in_specs=in_specs, out_specs=out_specs, check_vma=False)
```
